32 devices in a mesh: row: 8 (over z, x), col: 4 (over y, core).
Axes of the slice: x: 2, y: 2, z: 4, core: 2. Of those that a mesh axis runs over, the one named last changes fastest.
Arguments:
- normal_matrix: float32 [4096, 4096], P('row', 'col'), as said below
Outputs:
- factored: float32 [4096, 4096], P('row', 'col')
- log_det: float32 [], replicated
Inputs may be any that keep to these rules, and one draw needn't show every extreme that they name: normal_matrix is symmetric and positive definite.
All inputs are finite; a program needn't handle non-finite values.
Results may differ from the reference program's by a relative error of at most 0.0001.
Values sent between devices are 32-bit elements; how exact they have to be, the bound alone decides.
A program may use at most 64 MiB of HBM per device.

```python
import math
import jax
import jax.numpy as jnp
from jax import lax

B = 512
STEPS = 1
N = 4096


def draw_normal_matrix(key, part):
    key_green = jax.random.fold_in(key, 21)
    key_diag = jax.random.fold_in(key, 22)
    key_scale = jax.random.fold_in(key, 23)
    key_weight = jax.random.fold_in(key, 24)
    observe = 2 * B
    position = jnp.arange(N, dtype=jnp.float32) / N
    rising = jnp.exp(position * math.log(3.0))
    green = jax.random.normal(key_green, (observe, N), jnp.float32)
    data_weight = jnp.exp(jax.random.uniform(key_weight, (observe,), jnp.float32, math.log(0.7), math.log(1.4)))
    diag_add = jax.random.uniform(key_diag, (N,), jnp.float32, 0.5, 2.5)
    rough = jnp.exp(jax.random.uniform(key_scale, (N,), jnp.float32, 0.0, math.log(2.0)))
    scales = 0.6 * rising * rough
    weighted = green * (data_weight / math.sqrt(observe))[:, None]
    gram = jnp.dot(weighted.T, weighted, precision=lax.Precision.HIGHEST)
    base = 0.5 * (gram + gram.T) + jnp.diag(diag_add)
    return base * (scales[:, None] * scales[None, :])


def setup_inputs(seed: int = 0) -> dict:
    key_of = jax.random.split(jax.random.key(seed), 2)
    return {
        "normal_matrix": draw_normal_matrix(jax.random.fold_in(key_of[1], 71), 0),
    }


def reference(normal_matrix):
    matrix = normal_matrix
    log_det = jnp.float32(0.0)
    for panel_step in range(STEPS):
        start_at = panel_step * B
        end_at = start_at + B
        factor = jnp.linalg.cholesky(matrix[start_at:end_at, start_at:end_at])
        panel_cols = jax.scipy.linalg.solve_triangular(factor, matrix[end_at:, start_at:end_at].T, lower=True).T
        update = jnp.dot(panel_cols, panel_cols.T, precision=lax.Precision.HIGHEST)
        matrix = matrix.at[end_at:, end_at:].add(-update)
        matrix = matrix.at[end_at:, start_at:end_at].set(panel_cols)
        matrix = matrix.at[start_at:end_at, start_at:end_at].set(factor)
        matrix = matrix.at[start_at:end_at, end_at:].set(jnp.float32(0.0))
        log_det = log_det + 2.0 * jnp.sum(jnp.log(jnp.diagonal(factor)))
    return (matrix, log_det)
```

```python
import functools

import jax
import jax.numpy as jnp
from jax import lax
from jax.experimental import pallas as pl
from jax.experimental.pallas import tpu as pltpu
from jax.sharding import PartitionSpec as P

MESH = pl.DeviceIdType.MESH
NB = 128
CHUNKS = 32
SLOTS = 8
LEAD = 6
LAG = 10
STARTS = 4
PANELS = 8
VMEM = pl.BlockSpec(memory_space=pltpu.VMEM)


def dot_nt(a, b):
    return lax.dot_general(
        a, b, (((1,), (1,)), ((), ())), precision=lax.Precision.HIGHEST,
        preferred_element_type=jnp.float32,
    )


def dot_nn(a, b):
    return lax.dot_general(
        a, b, (((1,), (0,)), ((), ())), precision=lax.Precision.HIGHEST,
        preferred_element_type=jnp.float32,
    )


def split(a):
    high = a.astype(jnp.bfloat16)
    return high, (a - high.astype(jnp.float32)).astype(jnp.bfloat16)


def dot_split(a, b, axis):
    def dot(u, v):
        return lax.dot_general(u, v, (((1,), (axis,)), ((), ())), preferred_element_type=jnp.float32)

    return dot(a[0], b[0]) + (dot(a[0], b[1]) + dot(a[1], b[0]))


def factor_block(a, hook):
    groups = NB // 8
    lane = lax.broadcasted_iota(jnp.int32, (8, NB), 1)
    sub = lax.broadcasted_iota(jnp.int32, (8, NB), 0)
    left = [a[8 * g : 8 * g + 8, :] for g in range(groups)]
    right = [(lane == sub + 8 * g).astype(jnp.float32) for g in range(groups)]
    upper, inverse, pivots = [], [], []

    def row(x, t):
        return jnp.broadcast_to(x[t : t + 1, :], (8, NB))

    def column(x, t):
        return jnp.broadcast_to(x[:, t : t + 1], (8, NB))

    for p in range(groups):
        if p and p % (groups // SLOTS) == 0:
            hook(p // (groups // SLOTS) - 1)
        first = 8 * p
        v, i = left[p], right[p]
        cols = [column(v, first + t) for t in range(8)]
        mult = {g: [column(left[g], first + t) for t in range(8)] for g in range(p + 1, groups)}
        u_rows, i_rows, d_rows = v, i, cols[0]
        for t in range(8):
            here = sub == t
            pivot = row(cols[t], t)
            if t:
                u_rows = jnp.where(here, v, u_rows)
                i_rows = jnp.where(here, i, i_rows)
            d_rows = jnp.where(here, pivot, d_rows)
            recip = 1.0 / pivot
            factor = jnp.where(here, -recip, cols[t] * recip)
            for u in range(t + 1, 8):
                cols[u] = jnp.where(here, 0.0, cols[u]) - factor * row(cols[u], t)
            v = jnp.where(here, 0.0, v) - factor * row(v, t)
            i = jnp.where(here, 0.0, i) - factor * row(i, t)
        scale = lax.rsqrt(d_rows)
        upper.append(jnp.where(lane >= sub + first, u_rows * scale, 0.0))
        inverse.append(i_rows * scale)
        pivots.append(d_rows)
        v_rows = [row(v, t) for t in range(8)]
        i_rows = [row(i, t) for t in range(8)]
        for g in range(p + 1, groups):
            left_sum = mult[g][0] * v_rows[0]
            right_sum = mult[g][0] * i_rows[0]
            for t in range(1, 8):
                left_sum = left_sum + mult[g][t] * v_rows[t]
                right_sum = right_sum + mult[g][t] * i_rows[t]
            left[g] = left[g] - left_sum
            right[g] = right[g] - right_sum
    return jnp.concatenate(upper, 0), jnp.concatenate(inverse, 0), jnp.concatenate(pivots, 0)


def factor_all(a_ref, l_ref, w_ref, logdet_ref, work, upper, inverse, pivot, slot):
    size = a_ref.shape[0]
    work[:NB, :NB] = a_ref[:NB, :NB]
    l_ref[...] = jnp.zeros_like(l_ref)
    w_ref[...] = jnp.zeros_like(w_ref)

    @pl.loop(0, size // NB)
    def _(step):
        span = pl.ds(pl.multiple_of(step * NB, NB), NB)
        r, w, d = factor_block(work[span, span], lambda n: slot(step, n))
        upper[...] = r
        inverse[...] = w
        pivot[span, :] = d
        w_ref[span, span] = inverse[...]
        l_ref[span, span] = upper[...].T
        slot(step, SLOTS - 1)
        for p in range(size // NB):

            @pl.when(step == p)
            def _():
                at = slice(p * NB, (p + 1) * NB)
                end = (p + 1) * NB
                if p:
                    inner = dot_nn(l_ref[at, : p * NB], w_ref[: p * NB, : p * NB])
                    w_ref[at, : p * NB] = -dot_nn(inverse[...], inner)
                if end < size:
                    below = work[end:, at] if p else a_ref[end:, at]
                    l_ref[end:, at] = dot_nt(below, inverse[...])
                    following = slice(end, end + NB)
                    work[end:, following] = a_ref[end:, following] - dot_nt(l_ref[end:, :end], l_ref[following, :end])

    logdet_ref[...] = jnp.sum(jnp.log(pivot[...]), axis=0, keepdims=True)


def update_kernel(mine_ref, panel_ref, other_ref, l_ref, out_ref):
    r, c = lax.axis_index("row"), lax.axis_index("col")
    leading = (c == 0) & (pl.program_id(0) == 0)

    @pl.when(r == 0)
    def _():
        out_ref[...] = jnp.where(leading, l_ref[...], 0.0)

    @pl.when((r > 0) & leading)
    def _():
        out_ref[...] = panel_ref[...]

    @pl.when((r > 0) & jnp.logical_not(leading))
    def _():
        out_ref[...] = mine_ref[...] - dot_split(split(panel_ref[...]), split(other_ref[...]), 0)


def panel_kernel(mine_ref, panel_ref, other_ref, l_ref, logdet_ref, own_ref, cols_ref, w_ref, diag_ref, work, upper, inverse, pivot,
                 diag_send, diag_recv, own_send, own_recv, cols_send, cols_recv):
    rows, columns = lax.axis_size("row"), lax.axis_size("col")
    r, c = lax.axis_index("row"), lax.axis_index("col")
    q, x = r // 2, r % 2
    other = r + 1 - 2 * x
    partner = c + 1 - 2 * (c % 2)
    odd = c % 2 == 1
    width = own_ref.shape[0]
    top = r == 0
    corner = top & (c == 0)

    links = [
        ((r, partner), partner >= 0), ((other, c), other >= 0),
        ((r - 2, c), r >= 2), ((r + 2, c), r + 2 < rows),
        ((r, c - 2), c >= 2), ((r, c + 2), c + 2 < columns),
    ]
    barrier = pltpu.get_barrier_semaphore()
    for device, exists in links:
        @pl.when(exists)
        def _():
            pl.semaphore_signal(barrier, inc=1, device_id=device, device_id_type=MESH)
    peers = sum(jnp.where(exists, 1, 0).astype(jnp.int32) for _, exists in links)
    pl.semaphore_wait(barrier, peers)

    def send(source, target, send_sem, recv_sem, device):
        return pltpu.make_async_remote_copy(
            src_ref=source, dst_ref=target, send_sem=send_sem, recv_sem=recv_sem,
            device_id=device, device_id_type=MESH,
        )

    def start(condition, copies):
        for exists, copy in copies:
            @pl.when(condition & exists)
            def _():
                copy.start()

    def drain(condition, copies):
        for exists, copy in copies:
            @pl.when(condition & exists)
            def _():
                copy.wait_send()

    tall = NB // STARTS
    tiles = [(pl.ds(i * tall, tall), pl.ds(0, NB)) for i in range(STARTS)]
    tiles += [
        (pl.ds(i * NB, NB), pl.ds(j * NB, NB)) for j in range(width // NB) for i in range(j, width // NB) if i
    ]
    side_row = jnp.where(x == 0, r + 1, r - 2)
    has_side = ((x == 0) & (q >= 1)) | (r == 3)

    def diag_load(k):
        return pltpu.make_async_copy(mine_ref.at[tiles[k]], diag_ref.at[tiles[k]], diag_recv.at[k])

    def diag_copies(k):
        tile = diag_ref.at[tiles[k]]

        def to(n, device):
            return send(tile, tile, diag_send.at[n, k], diag_recv.at[k], device)

        return [
            ((c == 1) & (x == 0) & (r + 2 < rows), to(0, (r + 2, c))),
            ((c == 1) & has_side, to(1, (side_row, c))),
            (odd & (c + 2 < columns), to(2, (r, c + 2))),
            (odd & jnp.logical_not(top & (c == 1)), to(3, (r, c - 1))),
        ]

    def diag_first(k):
        return send(mine_ref.at[tiles[k]], diag_ref.at[tiles[k]], diag_send.at[0, k], diag_recv.at[k], (r, c + 1))

    def diag_step(k):
        @pl.when(corner)
        def _():
            diag_load(k).wait()

        @pl.when(jnp.logical_not(corner))
        def _():
            diag_copies(k)[0][1].wait_recv()

        start(odd, diag_copies(k))

    deep = width // PANELS
    everyone = pl.ds(0, width)

    def own_part(j):
        return own_ref.at[pl.ds(pl.multiple_of(j * deep, deep), deep), :]

    def own_copies(j, source):
        return [
            (c + 2 < columns, send(source, own_part(j), own_send.at[0, j], own_recv.at[j], (r, c + 2))),
            (c >= 0, send(source, own_part(j), own_send.at[1, j], own_recv.at[j], (r, c + 1))),
        ]

    def own_source(j):
        return mine_ref.at[pl.ds(pl.multiple_of(j * deep, deep), deep), everyone]

    def own_load(j):
        return pltpu.make_async_copy(own_source(j), own_part(j), own_recv.at[j])

    def own_relay(j):
        own_copies(j, own_part(j))[0][1].wait_recv()
        start(c >= 0, own_copies(j, own_part(j)))

    below = jnp.logical_not(top)
    own_relays = below & (c > 0) & jnp.logical_not(odd)

    piece = width // CHUNKS

    def cols_part(ref, half, i):
        return ref.at[pl.ds(pl.multiple_of(i * piece, piece), piece), pl.ds(half * width, width)]

    def cols_copies(half, i, source):
        def to(n, device):
            return send(source, cols_part(cols_ref, half, i), cols_send.at[2 * half + n, i], cols_recv.at[half, i], device)

        if half == 0:
            return [((x == 0) & (r + 2 < rows), to(0, (r + 2, c))), (has_side, to(1, (side_row, c)))]
        return [((x == 1) & (r + 2 < rows), to(0, (r + 2, c))), ((x == 1) & (q >= 1), to(1, (r - 1, c)))]

    def cols_first(half, i):
        source = cols_part(mine_ref, half, i)
        if half == 0:
            return cols_copies(0, i, source)[0][1]
        return send(source, cols_part(cols_ref, 1, i), cols_send.at[2, i], cols_recv.at[1, i], (r + 1, c))

    def cols_start(condition):
        @pl.when(condition)
        def _():
            @pl.loop(0, CHUNKS)
            def _(i):
                cols_first(1, i).start()

                @pl.when(c > 0)
                def _():
                    cols_first(0, i).start()

    def cols_wait(half, i):
        cols_copies(half, i, cols_part(cols_ref, half, i))[0][1].wait_recv()

    def cols_relay(half, i, condition):
        @pl.when(condition)
        def _():
            cols_wait(half, i)
            start(c >= 0, cols_copies(half, i, cols_part(cols_ref, half, i)))

    relays = [below & (c > 0) & (((x == 0) & (q >= 1)) | (r == 3)), x == 1]
    lead = jnp.where(r == 1, LEAD, 0)

    @pl.when(corner)
    def _():
        for k in range(len(tiles)):
            diag_first(k).start()
        for k in range(len(tiles)):
            diag_load(k).start()

    cols_start(top & (c != 1))

    @pl.when(below & (c == 0))
    def _():
        for j in range(PANELS):
            start(c >= 0, own_copies(j, own_source(j)))
        for j in range(PANELS):
            own_load(j).start()

    @pl.when(r == 1)
    def _():
        @pl.loop(0, LEAD)
        def _(i):
            cols_relay(1, i, x == 1)

    for k in range(STARTS):
        diag_step(k)

    early = top & (c <= 1)

    @pl.when(early)
    def _():
        for k in range(STARTS, len(tiles)):
            diag_step(k)

    cols_start(top & (c == 1))

    when = {(0, 0): 0, (0, 1): 1, (0, 2): 2, (0, 3): 3, (0, 4): 4, (0, 5): 5, (1, 0): 6, (1, 2): 7, (1, 4): 8}

    def slot(step, n):
        for (at_step, at_n), k in when.items():
            if at_n == n:
                @pl.when((step == at_step) & jnp.logical_not(early))
                def _():
                    diag_step(STARTS + k)
        at = SLOTS * step + n
        i = at + lead
        pair = 2 * (at - LAG)
        first = jnp.where(c == 1, pair, at)
        cols_relay(1, i, relays[1] & (i < CHUNKS))
        cols_relay(0, first, relays[0] & (first >= 0) & (first < CHUNKS))
        cols_relay(0, pair + 1, relays[0] & (c == 1) & (pair >= 0) & (pair < CHUNKS))
        if n % 2 == 1:
            j = (at - LAG - 1) // 2

            @pl.when(own_relays & (at > LAG) & (j < PANELS))
            def _():
                own_relay(j)

    factor_all(diag_ref, l_ref, w_ref, logdet_ref, work, upper, inverse, pivot, slot)

    @pl.when(below)
    def _():
        @pl.when(c == 0)
        def _():
            for j in range(PANELS):
                own_load(j).wait()

        @pl.when(odd)
        def _():
            for j in range(PANELS):
                own_copies(j, own_part(j))[0][1].wait_recv()

        half = width // 2
        own = split(own_ref[...])
        for e in range(half, width + 1, half):
            factor = split(w_ref[e - half : e, :e])
            panel_ref[:, e - half : e] = dot_split((own[0][:, :e], own[1][:, :e]), factor, 1)

        for n in range(2):
            @pl.when(jnp.logical_not(relays[n]) & ((c > 0) | (n == 1)))
            def _():
                @pl.loop(0, CHUNKS)
                def _(i):
                    cols_wait(n, i)

        cols = split(cols_ref[...])
        for e in range(half, width + 1, half):
            factor = split(w_ref[e - half : e, :e])
            other_ref[e - half : e, :] = dot_split(factor, (cols[0][:e, :], cols[1][:e, :]), 0)

    @pl.when(corner)
    def _():
        for k in range(len(tiles)):
            diag_first(k).wait_send()

    for k in range(len(tiles)):
        drain(odd, diag_copies(k))

    @pl.when(below & jnp.logical_not(odd))
    def _():
        @pl.loop(0, PANELS)
        def _(j):
            drain(c >= 0, own_copies(j, own_part(j)))

    @pl.loop(0, CHUNKS)
    def _(i):
        @pl.when(top)
        def _():
            cols_first(1, i).wait_send()

            @pl.when(c > 0)
            def _():
                cols_first(0, i).wait_send()

        for n in range(2):
            drain(relays[n], cols_copies(n, i, cols_part(cols_ref, n, i)))


def panel_step(mine):
    width = mine.shape[0]
    square = jax.ShapeDtypeStruct((width, width), jnp.float32)
    wide = (width, 2 * width)
    dma = pltpu.SemaphoreType.DMA
    tiles = (width // NB) * (width // NB + 1) // 2 - 1 + STARTS
    return pl.pallas_call(
        panel_kernel,
        out_shape=(
            square, jax.ShapeDtypeStruct(wide, jnp.float32), square,
            jax.ShapeDtypeStruct((1, NB), jnp.float32),
        ),
        in_specs=[pl.BlockSpec(memory_space=pl.ANY)],
        out_specs=(VMEM,) * 4,
        scratch_shapes=[
            pltpu.VMEM((width, width), jnp.float32), pltpu.VMEM(wide, jnp.float32),
            pltpu.VMEM((width, width), jnp.float32), pltpu.VMEM((width, width), jnp.float32),
            pltpu.VMEM((width, width), jnp.float32),
            pltpu.VMEM((NB, NB), jnp.float32), pltpu.VMEM((NB, NB), jnp.float32),
            pltpu.VMEM((width, NB), jnp.float32),
            dma((4, tiles)), dma((tiles,)), dma((2, PANELS)), dma((PANELS,)), dma((4, CHUNKS)), dma((2, CHUNKS)),
        ],
        compiler_params=pltpu.CompilerParams(collective_id=0, has_side_effects=True),
    )(mine)


def per_device(mine):
    panel, other, l, logdet = panel_step(mine)
    width = mine.shape[0]
    across = pl.BlockSpec((width, width), lambda s: (0, s))
    whole = pl.BlockSpec((width, width), lambda s: (0, 0))
    block = pl.pallas_call(
        update_kernel,
        grid=(mine.shape[1] // width,),
        out_shape=jax.ShapeDtypeStruct(mine.shape, jnp.float32),
        in_specs=[across, whole, across, whole],
        out_specs=across,
    )(mine, panel, other, l)
    return block, logdet[0, 0]


def solution(mesh):
    return jax.shard_map(
        per_device, mesh=mesh, in_specs=(P("row", "col"),), out_specs=(P("row", "col"), P()), check_vma=False
    )
```

```python
import functools

import jax
import jax.numpy as jnp
from jax import lax
from jax.experimental import pallas as pl
from jax.experimental.pallas import tpu as pltpu
from jax.sharding import PartitionSpec as P

MESH = pl.DeviceIdType.MESH
NB = 128
BAND = 32
CHUNKS = 32
SLOTS = 8
LEAD = 8
AHEAD = 3
LAG = 10
STARTS = 4
PANELS = 8
FIRST = 7
HOP = 6
LATEST = 15
VMEM = pl.BlockSpec(memory_space=pltpu.VMEM)


def split(a):
    high = a.astype(jnp.bfloat16)
    return high, (a - high.astype(jnp.float32)).astype(jnp.bfloat16)


def dot_split(a, b, axis):
    def dot(u, v):
        return lax.dot_general(u, v, (((1,), (axis,)), ((), ())), preferred_element_type=jnp.float32)

    return dot(a[0], b[0]) + (dot(a[0], b[1]) + dot(a[1], b[0]))


def dot_nt(a, b):
    return dot_split(split(a), split(b), 1)


def dot_nn(a, b):
    return dot_split(split(a), split(b), 0)


def total(terms):
    while len(terms) > 1:
        terms = [a + b for a, b in zip(terms[::2], terms[1::2])]
    return terms[0]


def eliminate(left, right, base, hook):
    sub = lax.broadcasted_iota(jnp.int32, (8, NB), 0)
    left, right = list(left), list(right)
    upper, inverse, pivots = [], [], []

    def row(x, t):
        return jnp.take_along_axis(x, jnp.full((8, NB), t, jnp.int32), axis=0)

    def column(x, t):
        return jnp.broadcast_to(x[:, t : t + 1], (8, NB))

    for p in range(0, len(left), 2):
        if p:
            hook()
        first = base + 8 * p
        rest = range(p + 2, len(left))
        cols = [[column(x, first + t) for x in left[p : p + 2]] for t in range(16)]
        mult = {g: [column(left[g], first + t) for t in range(16)] for g in rest}
        v, i = left[p : p + 2], right[p : p + 2]
        u_rows, i_rows, d_rows = list(v), list(i), [None, None]
        for t in range(16):
            at, s = t // 8, t % 8
            here = sub == s
            pivot = row(cols[t][at], s)
            if s:
                u_rows[at] = jnp.where(here, v[at], u_rows[at])
                i_rows[at] = jnp.where(here, i[at], i_rows[at])
                d_rows[at] = jnp.where(here, pivot, d_rows[at])
            else:
                u_rows[at], i_rows[at], d_rows[at] = v[at], i[at], pivot
            recip = 1.0 / pivot
            factor = [x * recip for x in cols[t]]
            factor[at] = jnp.where(here, -recip, factor[at])

            def step(pair):
                taken = row(pair[at], s)
                kept = [jnp.where(here, 0.0, x) if h == at else x for h, x in enumerate(pair)]
                return [x - f * taken for x, f in zip(kept, factor)]

            for w in range(t + 1, 16):
                cols[w] = step(cols[w])
            v, i = step(v), step(i)
        for h in range(2):
            scale = lax.rsqrt(d_rows[h])
            upper.append(u_rows[h] * scale)
            inverse.append(i_rows[h] * scale)
            pivots.append(d_rows[h])
        v_rows = [row(v[t // 8], t % 8) for t in range(16)]
        i_rows = [row(i[t // 8], t % 8) for t in range(16)]
        for g in rest:
            left[g] = left[g] - total([mult[g][t] * v_rows[t] for t in range(16)])
            right[g] = right[g] - total([mult[g][t] * i_rows[t] for t in range(16)])
    return upper, inverse, pivots


def factor_block(a, hook):
    lane = lax.broadcasted_iota(jnp.int32, (NB, NB), 1)
    sub = lax.broadcasted_iota(jnp.int32, (NB, NB), 0)
    left, right = a, (lane == sub).astype(jnp.float32)
    upper, inverse, pivots = [], [], []
    for base in range(0, NB, BAND):
        if base:
            hook()
        rows = [slice(8 * g, 8 * g + 8) for g in range(BAND // 8)]
        u, i, d = eliminate([left[x] for x in rows], [right[x] for x in rows], base, hook)
        u, i = jnp.concatenate(u, 0), jnp.concatenate(i, 0)
        upper.append(u)
        inverse.append(i)
        pivots += d
        if base + BAND < NB:
            change = dot_nn(u.T[base + BAND :, :], jnp.concatenate([u, i], 1))
            left, right = left[BAND:] - change[:, :NB], right[BAND:] - change[:, NB:]
    upper = jnp.where(lane >= sub, jnp.concatenate(upper, 0), 0.0)
    return upper, jnp.concatenate(inverse, 0), jnp.concatenate(pivots, 0)


def factor_all(a_ref, l_ref, w_ref, logdet_ref, work, upper, inverse, pivot, slot):
    size = a_ref.shape[0]
    work[:NB, :NB] = a_ref[:NB, :NB]
    l_ref[...] = jnp.zeros_like(l_ref)
    w_ref[...] = jnp.zeros_like(w_ref)

    @pl.loop(0, size // NB)
    def _(step):
        span = pl.ds(pl.multiple_of(step * NB, NB), NB)
        numbers = iter(range(SLOTS - 1))
        r, w, d = factor_block(work[span, span], lambda: slot(step, next(numbers)))
        upper[...] = r
        inverse[...] = w
        pivot[span, :] = d
        w_ref[span, span] = inverse[...]
        l_ref[span, span] = upper[...].T
        slot(step, SLOTS - 1)
        for p in range(size // NB):

            @pl.when(step == p)
            def _():
                at = slice(p * NB, (p + 1) * NB)
                end = (p + 1) * NB
                if p:
                    inner = dot_nn(l_ref[at, : p * NB], w_ref[: p * NB, : p * NB])
                    w_ref[at, : p * NB] = -dot_nn(inverse[...], inner)
                if end < size:
                    below = work[end:, at] if p else a_ref[end:, at]
                    l_ref[end:, at] = dot_nt(below, inverse[...])
                    following = slice(end, end + NB)
                    work[end:, following] = a_ref[end:, following] - dot_nt(l_ref[end:, :end], l_ref[following, :end])

    logdet_ref[...] = jnp.sum(jnp.log(pivot[...]), axis=0, keepdims=True)


def update_kernel(rest_ref, panel_ref, other_ref, l_ref, out_ref):
    r, c = lax.axis_index("row"), lax.axis_index("col")
    leading = (c == 0) & (pl.program_id(0) == 0)

    @pl.when(r == 0)
    def _():
        out_ref[...] = jnp.where(leading, l_ref[...], 0.0)

    @pl.when((r > 0) & leading)
    def _():
        out_ref[...] = panel_ref[...]

    @pl.when((r > 0) & jnp.logical_not(leading))
    def _():
        half = panel_ref.shape[1] // 2
        out_ref[...] = rest_ref[...] - dot_nn(panel_ref[:, half:], other_ref[half:, :])


def panel_kernel(mine_ref, panel_ref, other_ref, rest_ref, l_ref, logdet_ref, own_ref, cols_ref, w_ref, diag_ref, work, upper, inverse, pivot,
                 diag_send, diag_recv, own_send, own_recv, cols_send, cols_recv):
    rows, columns = lax.axis_size("row"), lax.axis_size("col")
    r, c = lax.axis_index("row"), lax.axis_index("col")
    q, x = r // 2, r % 2
    other = r + 1 - 2 * x
    partner = c + 1 - 2 * (c % 2)
    odd = c % 2 == 1
    width = own_ref.shape[0]
    top = r == 0
    corner = top & (c == 0)

    links = [
        ((r, partner), partner >= 0), ((other, c), other >= 0),
        ((r - 2, c), r >= 2), ((r + 2, c), r + 2 < rows),
        ((r, c - 2), c >= 2), ((r, c + 2), c + 2 < columns),
    ]
    barrier = pltpu.get_barrier_semaphore()
    for device, exists in links:
        @pl.when(exists)
        def _():
            pl.semaphore_signal(barrier, inc=1, device_id=device, device_id_type=MESH)
    peers = sum(jnp.where(exists, 1, 0).astype(jnp.int32) for _, exists in links)
    pl.semaphore_wait(barrier, peers)

    def send(source, target, send_sem, recv_sem, device):
        return pltpu.make_async_remote_copy(
            src_ref=source, dst_ref=target, send_sem=send_sem, recv_sem=recv_sem,
            device_id=device, device_id_type=MESH,
        )

    def start(condition, copies):
        for exists, copy in copies:
            @pl.when(condition & exists)
            def _():
                copy.start()

    def drain(condition, copies):
        for exists, copy in copies:
            @pl.when(condition & exists)
            def _():
                copy.wait_send()

    tall = NB // STARTS
    tiles = [(pl.ds(i * tall, tall), pl.ds(0, NB)) for i in range(STARTS)]
    tiles += [
        (pl.ds(i * NB, NB), pl.ds(j * NB, NB)) for j in range(width // NB) for i in range(j, width // NB) if i
    ]
    side_row = jnp.where(x == 0, r + 1, r - 2)
    has_side = ((x == 0) & (q >= 1)) | (r == 3)

    def diag_load(k):
        return pltpu.make_async_copy(mine_ref.at[tiles[k]], diag_ref.at[tiles[k]], diag_recv.at[k])

    def diag_copies(k):
        tile = diag_ref.at[tiles[k]]

        def to(n, device):
            return send(tile, tile, diag_send.at[n, k], diag_recv.at[k], device)

        return [
            ((c == 1) & (x == 0) & (r + 2 < rows), to(0, (r + 2, c))),
            ((c == 1) & has_side, to(1, (side_row, c))),
            (odd & (c + 2 < columns), to(2, (r, c + 2))),
            (odd & jnp.logical_not(top & (c == 1)), to(3, (r, c - 1))),
        ]

    def diag_first(k):
        return send(mine_ref.at[tiles[k]], diag_ref.at[tiles[k]], diag_send.at[0, k], diag_recv.at[k], (r, c + 1))

    def diag_step(k):
        @pl.when(corner)
        def _():
            diag_load(k).wait()

        @pl.when(jnp.logical_not(corner))
        def _():
            diag_copies(k)[0][1].wait_recv()

        start(odd, diag_copies(k))

    deep = width // PANELS
    everyone = pl.ds(0, width)

    def own_part(j):
        return own_ref.at[pl.ds(pl.multiple_of(j * deep, deep), deep), :]

    def own_copies(j, source):
        return [
            (c + 2 < columns, send(source, own_part(j), own_send.at[0, j], own_recv.at[j], (r, c + 2))),
            (c >= 0, send(source, own_part(j), own_send.at[1, j], own_recv.at[j], (r, c + 1))),
        ]

    def own_source(j):
        return mine_ref.at[pl.ds(pl.multiple_of(j * deep, deep), deep), everyone]

    def own_load(j):
        return pltpu.make_async_copy(own_source(j), own_part(j), own_recv.at[j])

    def own_relay(j):
        own_copies(j, own_part(j))[0][1].wait_recv()
        start(c >= 0, own_copies(j, own_part(j)))

    below = jnp.logical_not(top)
    own_relays = below & (c > 0) & jnp.logical_not(odd)
    own_lag = jnp.minimum(FIRST + HOP * (c // 2), LATEST)

    piece = width // CHUNKS

    def cols_part(ref, half, i):
        return ref.at[pl.ds(pl.multiple_of(i * piece, piece), piece), pl.ds(half * width, width)]

    def cols_copies(half, i, source):
        def to(n, device):
            return send(source, cols_part(cols_ref, half, i), cols_send.at[2 * half + n, i], cols_recv.at[half, i], device)

        if half == 0:
            return [((x == 0) & (r + 2 < rows), to(0, (r + 2, c))), (has_side, to(1, (side_row, c)))]
        return [((x == 1) & (r + 2 < rows), to(0, (r + 2, c))), ((x == 1) & (q >= 1), to(1, (r - 1, c)))]

    def cols_first(half, i):
        source = cols_part(mine_ref, half, i)
        if half == 0:
            return cols_copies(0, i, source)[0][1]
        return send(source, cols_part(cols_ref, 1, i), cols_send.at[2, i], cols_recv.at[1, i], (r + 1, c))

    def cols_start(condition):
        @pl.when(condition)
        def _():
            @pl.loop(0, CHUNKS)
            def _(i):
                cols_first(1, i).start()

                @pl.when(c > 0)
                def _():
                    cols_first(0, i).start()

    def cols_wait(half, i):
        cols_copies(half, i, cols_part(cols_ref, half, i))[0][1].wait_recv()

    def cols_relay(half, i, condition):
        @pl.when(condition)
        def _():
            cols_wait(half, i)
            start(c >= 0, cols_copies(half, i, cols_part(cols_ref, half, i)))

    relays = [below & (c > 0) & (((x == 0) & (q >= 1)) | (r == 3)), x == 1]
    lead = jnp.where(r == 1, LEAD, jnp.where(c > 1, AHEAD, 0))
    lead_left = jnp.where(c > 1, AHEAD, 0)

    @pl.when(corner)
    def _():
        for k in range(len(tiles)):
            diag_first(k).start()
        for k in range(len(tiles)):
            diag_load(k).start()

    cols_start(top & (c != 1))

    @pl.when(below & (c == 0))
    def _():
        for j in range(PANELS):
            own_load(j).start()

    @pl.loop(0, LEAD)
    def _(i):
        cols_relay(1, i, relays[1] & (i < lead))
        cols_relay(0, i, relays[0] & (i < lead_left))

    for k in range(STARTS):
        diag_step(k)

    early = top & (c <= 1)

    @pl.when(early)
    def _():
        for k in range(STARTS, len(tiles)):
            diag_step(k)

    cols_start(top & (c == 1))

    when = {(0, 0): 0, (0, 1): 1, (0, 2): 2, (0, 3): 3, (0, 4): 4, (0, 5): 5, (1, 0): 6, (1, 2): 7, (1, 4): 8}

    def slot(step, n):
        for (at_step, at_n), k in when.items():
            if at_n == n:
                @pl.when((step == at_step) & jnp.logical_not(early))
                def _():
                    diag_step(STARTS + k)
        at = SLOTS * step + n
        i = at + lead
        pair = 2 * (at - LAG)
        first = jnp.where(c == 1, pair, at + lead_left)
        cols_relay(1, i, relays[1] & (i < CHUNKS))
        cols_relay(0, first, relays[0] & (first >= 0) & (first < CHUNKS))
        cols_relay(0, pair + 1, relays[0] & (c == 1) & (pair >= 0) & (pair < CHUNKS))
        if n % 2 == 1:
            j = (at - own_lag) // 2

            @pl.when(below & (c == 0) & (at >= own_lag) & (j < PANELS))
            def _():
                start(c >= 0, own_copies(j, own_source(j)))

            @pl.when(own_relays & (at >= own_lag) & (j < PANELS))
            def _():
                own_relay(j)

    factor_all(diag_ref, l_ref, w_ref, logdet_ref, work, upper, inverse, pivot, slot)

    @pl.when(below)
    def _():
        @pl.when(c == 0)
        def _():
            for j in range(PANELS):
                own_load(j).wait()

        @pl.when(odd)
        def _():
            for j in range(PANELS):
                own_copies(j, own_part(j))[0][1].wait_recv()

        half = width // 2
        own = split(own_ref[...])

        def panel(e):
            factor = split(w_ref[e - half : e, :e])
            panel_ref[:, e - half : e] = dot_split((own[0][:, :e], own[1][:, :e]), factor, 1)

        def block_row(e):
            for n in range(2):
                @pl.when(jnp.logical_not(relays[n]) & ((c > 0) | (n == 1)))
                def _():
                    @pl.loop((e - half) // piece, e // piece)
                    def _(i):
                        cols_wait(n, i)

            other_ref[e - half : e, :] = dot_split(split(w_ref[e - half : e, :e]), split(cols_ref[:e, :]), 0)

        panel(half)
        block_row(half)
        rest_ref[...] = mine_ref[...] - dot_nn(panel_ref[:, :half], other_ref[:half, :])
        panel(width)
        block_row(width)

    @pl.when(corner)
    def _():
        for k in range(len(tiles)):
            diag_first(k).wait_send()

    for k in range(len(tiles)):
        drain(odd, diag_copies(k))

    @pl.when(below & jnp.logical_not(odd))
    def _():
        @pl.loop(0, PANELS)
        def _(j):
            drain(c >= 0, own_copies(j, own_part(j)))

    @pl.loop(0, CHUNKS)
    def _(i):
        @pl.when(top)
        def _():
            cols_first(1, i).wait_send()

            @pl.when(c > 0)
            def _():
                cols_first(0, i).wait_send()

        for n in range(2):
            drain(relays[n], cols_copies(n, i, cols_part(cols_ref, n, i)))


def panel_step(mine):
    width = mine.shape[0]
    square = jax.ShapeDtypeStruct((width, width), jnp.float32)
    wide = (width, 2 * width)
    dma = pltpu.SemaphoreType.DMA
    tiles = (width // NB) * (width // NB + 1) // 2 - 1 + STARTS
    return pl.pallas_call(
        panel_kernel,
        out_shape=(
            square, jax.ShapeDtypeStruct(wide, jnp.float32), jax.ShapeDtypeStruct(wide, jnp.float32), square,
            jax.ShapeDtypeStruct((1, NB), jnp.float32),
        ),
        in_specs=[VMEM],
        out_specs=(VMEM,) * 5,
        scratch_shapes=[
            pltpu.VMEM((width, width), jnp.float32), pltpu.VMEM(wide, jnp.float32),
            pltpu.VMEM((width, width), jnp.float32), pltpu.VMEM((width, width), jnp.float32),
            pltpu.VMEM((width, width), jnp.float32),
            pltpu.VMEM((NB, NB), jnp.float32), pltpu.VMEM((NB, NB), jnp.float32),
            pltpu.VMEM((width, NB), jnp.float32),
            dma((4, tiles)), dma((tiles,)), dma((2, PANELS)), dma((PANELS,)), dma((4, CHUNKS)), dma((2, CHUNKS)),
        ],
        compiler_params=pltpu.CompilerParams(collective_id=0, has_side_effects=True, vmem_limit_bytes=28 << 20),
    )(mine)


def per_device(mine):
    panel, other, rest, l, logdet = panel_step(mine)
    width = mine.shape[0]
    across = pl.BlockSpec((width, width), lambda s: (0, s))
    whole = pl.BlockSpec((width, width), lambda s: (0, 0))
    block = pl.pallas_call(
        update_kernel,
        grid=(mine.shape[1] // width,),
        out_shape=jax.ShapeDtypeStruct(mine.shape, jnp.float32),
        in_specs=[across, whole, across, whole],
        out_specs=across,
        compiler_params=pltpu.CompilerParams(vmem_limit_bytes=16 << 20),
    )(rest, panel, other, l)
    return block, logdet[0, 0]


def solution(mesh):
    return jax.shard_map(
        per_device, mesh=mesh, in_specs=(P("row", "col"),), out_specs=(P("row", "col"), P()), check_vma=False
    )
```

```python
import functools

import jax
import jax.numpy as jnp
from jax import lax
from jax.experimental import pallas as pl
from jax.experimental.pallas import tpu as pltpu
from jax.sharding import PartitionSpec as P

MESH = pl.DeviceIdType.MESH
NB = 128
BAND = 32
CHUNKS = 32
LEAD = 8
AHEAD = 3
LAG = 6
LATE = 14
STARTS = 4
PANELS = 16
FIRST = 9
MIDDLE = 22
HOP = 3
LAST = 12
VMEM = pl.BlockSpec(memory_space=pltpu.VMEM)


def split(a):
    high = a.astype(jnp.bfloat16)
    return high, (a - high.astype(jnp.float32)).astype(jnp.bfloat16)


def dot_split(a, b, axis):
    def dot(u, v):
        return lax.dot_general(u, v, (((1,), (axis,)), ((), ())), preferred_element_type=jnp.float32)

    return dot(a[0], b[0]) + (dot(a[0], b[1]) + dot(a[1], b[0]))


def dot_nt(a, b):
    return dot_split(split(a), split(b), 1)


def dot_nn(a, b):
    return dot_split(split(a), split(b), 0)


def total(terms):
    while len(terms) > 1:
        terms = [a + b for a, b in zip(terms[::2], terms[1::2])]
    return terms[0]


def eliminate(left, right, base):
    sub = lax.broadcasted_iota(jnp.int32, (8, NB), 0)
    left, right = list(left), list(right)
    upper, inverse = [], []

    def row(x, t):
        return jnp.take_along_axis(x, jnp.full((8, NB), t, jnp.int32), axis=0)

    def column(x, t):
        return jnp.broadcast_to(x[:, t : t + 1], (8, NB))

    for p in range(0, len(left), 2):
        first = base + 8 * p
        rest = range(p + 2, len(left))
        cols = [[column(x, first + t) for x in left[p : p + 2]] for t in range(16)]
        mult = {g: [column(left[g], first + t) for t in range(16)] for g in rest}
        v, i = left[p : p + 2], right[p : p + 2]
        u_rows, i_rows, d_rows = list(v), list(i), [None, None]
        for t in range(16):
            at, s = t // 8, t % 8
            here = sub == s
            pivot = row(cols[t][at], s)
            if s:
                u_rows[at] = jnp.where(here, v[at], u_rows[at])
                i_rows[at] = jnp.where(here, i[at], i_rows[at])
                d_rows[at] = jnp.where(here, pivot, d_rows[at])
            else:
                u_rows[at], i_rows[at], d_rows[at] = v[at], i[at], pivot
            recip = 1.0 / pivot
            factor = [x * recip for x in cols[t]]
            factor[at] = jnp.where(here, -recip, factor[at])

            def step(pair):
                taken = row(pair[at], s)
                kept = [jnp.where(here, 0.0, x) if h == at else x for h, x in enumerate(pair)]
                return [x - f * taken for x, f in zip(kept, factor)]

            for w in range(t + 1, 16):
                cols[w] = step(cols[w])
            v, i = step(v), step(i)
        for h in range(2):
            scale = lax.rsqrt(d_rows[h])
            upper.append(u_rows[h] * scale)
            inverse.append(i_rows[h] * scale)
        v_rows = [row(v[t // 8], t % 8) for t in range(16)]
        i_rows = [row(i[t // 8], t % 8) for t in range(16)]
        for g in rest:
            left[g] = left[g] - total([mult[g][t] * v_rows[t] for t in range(16)])
            right[g] = right[g] - total([mult[g][t] * i_rows[t] for t in range(16)])
    return upper, inverse


def factor_block(a):
    lane = lax.broadcasted_iota(jnp.int32, (NB, NB), 1)
    sub = lax.broadcasted_iota(jnp.int32, (NB, NB), 0)
    left, right = a, (lane == sub).astype(jnp.float32)
    upper, inverse = [], []
    for base in range(0, NB, BAND):
        rows = [slice(8 * g, 8 * g + 8) for g in range(BAND // 8)]
        u, i = eliminate([left[x] for x in rows], [right[x] for x in rows], base)
        u, i = jnp.concatenate(u, 0), jnp.concatenate(i, 0)
        upper.append(u)
        inverse.append(i)
        if base + BAND < NB:
            change = dot_nn(u.T[base + BAND :, :], jnp.concatenate([u, i], 1))
            left, right = left[BAND:] - change[:, :NB], right[BAND:] - change[:, NB:]
    upper = jnp.where(lane >= sub, jnp.concatenate(upper, 0), 0.0)
    return upper, jnp.concatenate(inverse, 0)


def factor_all(a_ref, l_ref, w_ref, work, upper, inverse, arrive, leave):
    size = a_ref.shape[0]
    work[:NB, :NB] = a_ref[:NB, :NB]
    l_ref[...] = jnp.zeros_like(l_ref)
    w_ref[...] = jnp.zeros_like(w_ref)

    @pl.loop(0, size // NB)
    def _(step):
        span = pl.ds(pl.multiple_of(step * NB, NB), NB)
        r, w = factor_block(work[span, span])
        upper[...] = r
        inverse[...] = w
        w_ref[span, span] = inverse[...]
        l_ref[span, span] = upper[...].T
        for p in range(size // NB):

            @pl.when(step == p)
            def _():
                arrive(p)
                at = slice(p * NB, (p + 1) * NB)
                end = (p + 1) * NB
                if end < size:
                    below = work[end:, at] if p else a_ref[end:, at]
                    l_ref[end:, at] = dot_nt(below, inverse[...])
                    following = slice(end, end + NB)
                    work[end:, following] = a_ref[end:, following] - dot_nt(l_ref[end:, :end], l_ref[following, :end])
                if p:
                    inner = dot_nn(l_ref[at, : p * NB], w_ref[: p * NB, : p * NB])
                    w_ref[at, : p * NB] = -dot_nn(inverse[...], inner)
                    leave(p - 1)


def update_kernel(rest_ref, panel_ref, other_ref, l_ref, out_ref):
    r, c = lax.axis_index("row"), lax.axis_index("col")
    leading = (c == 0) & (pl.program_id(0) == 0)

    @pl.when(r == 0)
    def _():
        out_ref[...] = jnp.where(leading, l_ref[...], 0.0)

    @pl.when((r > 0) & leading)
    def _():
        out_ref[...] = panel_ref[...]

    @pl.when((r > 0) & jnp.logical_not(leading))
    def _():
        half = panel_ref.shape[1] // 2
        out_ref[...] = rest_ref[...] - dot_nn(panel_ref[:, half:], other_ref[half:, :])


def panel_kernel(mine_ref, panel_ref, other_ref, rest_ref, l_ref, logdet_ref,
                 own_ref, cols_ref, relay_ref, w_ref, diag_ref, work, upper, inverse,
                 diag_send, diag_recv, own_send, own_recv, cols_send, cols_recv, relay_send, relay_recv, w_send, w_recv):
    rows, columns = lax.axis_size("row"), lax.axis_size("col")
    r, c = lax.axis_index("row"), lax.axis_index("col")
    q, x = r // 2, r % 2
    other = r + 1 - 2 * x
    partner = c + 1 - 2 * (c % 2)
    odd = c % 2 == 1
    even = jnp.logical_not(odd)
    width = own_ref.shape[0]
    top = r == 0
    below = jnp.logical_not(top)
    corner = top & (c == 0)

    links = [
        ((r, partner), partner >= 0), ((other, c), odd),
        ((r - 2, c), odd & (r >= 2)), ((r + 2, c), odd & (r + 2 < rows)),
        ((r, c - 2), odd & (c >= 2)), ((r, c + 2), odd & (c + 2 < columns)),
        ((r + 1, partner), top & even), ((r + 2, partner), top & even),
        ((r - 1, partner), (r == 1) & odd), ((r - 2, partner), (r == 2) & odd),
    ]
    barrier = pltpu.get_barrier_semaphore()
    for device, exists in links:
        @pl.when(exists)
        def _():
            pl.semaphore_signal(barrier, inc=1, device_id=device, device_id_type=MESH)
    peers = sum(jnp.where(exists, 1, 0).astype(jnp.int32) for _, exists in links)
    pl.semaphore_wait(barrier, peers)

    def send(source, target, send_sem, recv_sem, device):
        return pltpu.make_async_remote_copy(
            src_ref=source, dst_ref=target, send_sem=send_sem, recv_sem=recv_sem,
            device_id=device, device_id_type=MESH,
        )

    def start(condition, copies):
        for exists, copy in copies:
            @pl.when(condition & exists)
            def _():
                copy.start()

    def drain(condition, copies):
        for exists, copy in copies:
            @pl.when(condition & exists)
            def _():
                copy.wait_send()

    side_row = jnp.where(x == 0, r + 1, r - 2)
    has_side = ((x == 0) & (q >= 1)) | (r == 3)

    tall = NB // STARTS
    tiles = [(pl.ds(i * tall, tall), pl.ds(0, NB)) for i in range(STARTS)]
    places = [(i, j) for j in range(width // NB) for i in range(j, width // NB) if i]
    tiles += [(pl.ds(i * NB, NB), pl.ds(j * NB, NB)) for i, j in places]

    def diag_load(k):
        return pltpu.make_async_copy(mine_ref.at[tiles[k]], diag_ref.at[tiles[k]], diag_recv.at[k])

    def diag_copies(k):
        tile = diag_ref.at[tiles[k]]

        def to(n, device):
            return send(tile, tile, diag_send.at[n, k], diag_recv.at[k], device)

        return [
            ((c == 1) & (x == 0) & (r + 2 < rows), to(0, (r + 2, c))),
            ((c == 1) & has_side, to(1, (side_row, c))),
            (c + 2 < columns, to(2, (r, c + 2))),
            (jnp.logical_not(top & (c == 1)), to(3, (r, c - 1))),
        ]

    def diag_first(k):
        return send(mine_ref.at[tiles[k]], diag_ref.at[tiles[k]], diag_send.at[0, k], diag_recv.at[k], (r, c + 1))

    def diag_relay(k):
        copies = diag_copies(k)
        copies[0][1].wait_recv()
        start(r >= 0, copies)

    def diag_wait(k):
        @pl.when(corner)
        def _():
            diag_load(k).wait()

        @pl.when(jnp.logical_not(corner))
        def _():
            diag_first(k).wait_recv()

    deep = width // PANELS

    def own_part(j):
        return own_ref.at[pl.ds(pl.multiple_of(j * deep, deep), deep), :]

    def own_source(j):
        return mine_ref.at[pl.ds(pl.multiple_of(j * deep, deep), deep), pl.ds(0, width)]

    def own_load(j):
        return pltpu.make_async_copy(own_source(j), own_part(j), own_recv.at[j])

    def own_first(j):
        return send(own_source(j), own_part(j), own_send.at[0, j], own_recv.at[j], (r, c + 1))

    def own_copies(j):
        part = own_part(j)

        def to(n, device):
            return send(part, part, own_send.at[n, j], own_recv.at[j], device)

        return [(c + 2 < columns, to(0, (r, c + 2))), (c > 1, to(1, (r, c - 1)))]

    def own_relay(j):
        copies = own_copies(j)
        copies[0][1].wait_recv()
        start(r >= 0, copies)

    piece = width // CHUNKS

    def cols_part(ref, half, i):
        return ref.at[pl.ds(pl.multiple_of(i * piece, piece), piece), pl.ds(half * width, width)]

    def routes(half):
        if half == 0:
            return [((x == 0) & (r + 2 < rows), (r + 2, c)), (has_side, (side_row, c))]
        return [((x == 1) & (r + 2 < rows), (r + 2, c)), ((x == 1) & (q >= 1), (r - 1, c))]

    def cols_first(half, i):
        return send(
            cols_part(mine_ref, half, i), cols_part(cols_ref, half, i), cols_send.at[half, i], cols_recv.at[half, i],
            (r + 2 - half, c),
        )

    def relay_first(half, i):
        return send(
            cols_part(mine_ref, half, i), cols_part(relay_ref, half, i), relay_send.at[half, i], relay_recv.at[half, i],
            (r + 2 - half, c + 1),
        )

    def cols_copies(half, i):
        part = cols_part(cols_ref, half, i)
        return [
            (exists, send(part, part, cols_send.at[2 * half + n, i], cols_recv.at[half, i], device))
            for n, (exists, device) in enumerate(routes(half))
        ]

    def relay_copies(half, i):
        part = cols_part(relay_ref, half, i)
        copies = [
            (exists, send(part, part, relay_send.at[3 * half + n, i], relay_recv.at[half, i], device))
            for n, (exists, device) in enumerate(routes(half))
        ]
        final = send(part, cols_part(cols_ref, half, i), relay_send.at[3 * half + 2, i], cols_recv.at[half, i], (r, c - 1))
        return copies + [(r >= 0, final)]

    def cols_relay(half, i):
        @pl.when((i >= 0) & (i < CHUNKS))
        def _():
            def pass_on(copies):
                copies[0][1].wait_recv()
                start(r >= 0, copies)

            if half == 0:
                @pl.when(c > 1)
                def _():
                    pass_on(relay_copies(0, i))
            else:
                pass_on(relay_copies(1, i))
            pass_on(cols_copies(half, i))

    def w_copy(p):
        part = w_ref.at[pl.ds(p * NB, NB), pl.ds(0, (p + 1) * NB)]
        return send(part, part, w_send.at[p], w_recv.at[p], (r, partner))

    steps = width // NB
    half = width // 2

    def log_det():
        here = lax.broadcasted_iota(jnp.int32, (NB, NB), 0) == lax.broadcasted_iota(jnp.int32, (NB, NB), 1)
        blocks = [slice(p * NB, (p + 1) * NB) for p in range(steps)]
        logs = sum(jnp.log(jnp.where(here, w_ref[at, at], 1.0)) for at in blocks)
        across = jnp.sum(logs, axis=0, keepdims=True)
        logdet_ref[...] = jnp.broadcast_to(-2.0 * jnp.sum(across, axis=1, keepdims=True), logdet_ref.shape)

    def panel(e, at=slice(None)):
        own = split(own_ref[at, :e])
        panel_ref[at, e - half : e] = dot_split(own, split(w_ref[e - half : e, :e]), 1)

    def block_row(e, at=slice(None)):
        other_ref[e - half : e, at] = dot_split(split(w_ref[e - half : e, :e]), split(cols_ref[:e, at]), 0)

    def update(at=slice(None)):
        rest_ref[:, at] = mine_ref[:, at] - dot_nn(panel_ref[:, :half], other_ref[:half, at])

    lower = [slice(i, i + half) for i in range(0, 2 * width, half)]

    def w_wait(first):
        for p in range(first, first + half // NB):
            w_copy(p).wait_recv()

    @pl.when(even)
    def _():
        @pl.when(corner)
        def _():
            for k in range(len(tiles)):
                diag_first(k).start()
            for k in range(len(tiles)):
                diag_load(k).start()

        @pl.when(top)
        def _():
            @pl.loop(0, CHUNKS)
            def _(i):
                relay_first(1, i).start()

                @pl.when(c > 0)
                def _():
                    relay_first(0, i).start()

        @pl.when(below & (c == 0))
        def _():
            for j in range(PANELS):
                own_first(j).start()
            for j in range(PANELS):
                own_load(j).start()

        for k in range(STARTS):
            diag_wait(k)

        def arrive(p):
            for k, (i, j) in enumerate(places):
                if (j == 0 and p == 0) or j == p + 1:
                    diag_wait(STARTS + k)

        factor_all(diag_ref, l_ref, w_ref, work, upper, inverse, arrive, lambda p: w_copy(p).start())
        log_det()

        @pl.when(below)
        def _():
            @pl.when(c == 0)
            def _():
                for j in range(PANELS):
                    own_load(j).wait()

            @pl.when(c > 0)
            def _():
                for j in range(PANELS):
                    own_first(j).wait_recv()

            panel(half)

        w_copy(steps - 1).start()

    @pl.when(odd)
    def _():
        for p in range(steps):
            if p * NB % half == 0 and half > NB:
                w_ref[p * NB : (p + 1) * NB, (p + 1) * NB : p * NB + half] = jnp.zeros((NB, half - NB), jnp.float32)

        @pl.when(top)
        def _():
            @pl.loop(0, CHUNKS)
            def _(i):
                cols_first(1, i).start()

                @pl.when(c > 1)
                def _():
                    cols_first(0, i).start()

        early = jnp.where(r == 1, LEAD, jnp.where(c > 1, AHEAD, 0))
        shift_a = jnp.where(r == 1, -LAG, 0) + jnp.where(c > 1, AHEAD, -LATE)
        shift_b = jnp.where(r == 1, LEAD, jnp.where(c > 1, AHEAD, 0)) - jnp.where(x == 0, LAG, 0)

        @pl.when(below)
        def _():
            @pl.loop(0, LEAD)
            def _(i):
                @pl.when(i < shift_b)
                def _():
                    cols_relay(1, i)

                @pl.when(i < shift_a)
                def _():
                    cols_relay(0, i)

        for k in range(STARTS):
            diag_relay(k)

        def turn(i):
            @pl.when(below)
            def _():
                cols_relay(1, i + shift_b)
                at = jnp.where(c > 1, i + shift_a, 2 * (i + shift_a))
                cols_relay(0, at)
                cols_relay(0, jnp.where(c > 1, CHUNKS, at + 1))
                j = i - jnp.minimum(FIRST + HOP * (c // 2), LAST)

                @pl.when((j >= 0) & (j < PANELS))
                def _():
                    own_relay(j)

        for k in range(len(places)):
            diag_relay(STARTS + k)
            turn(k)

        @pl.when(top & (c == 1))
        def _():
            @pl.loop(0, CHUNKS)
            def _(i):
                cols_first(0, i).start()

        @pl.loop(len(places), MIDDLE)
        def _(i):
            turn(i)

        w_wait(0)
        rows_of, left, right = lower[: width // half], lower[: width // half], lower[width // half :]
        work_items = [functools.partial(block_row, half, at) for at in right]
        work_items += [functools.partial(panel, half, rows_of[0]), None, None]
        work_items += [functools.partial(panel, half, at) for at in rows_of[1:]]
        work_items += [functools.partial(block_row, half, at) for at in left]
        work_items += [functools.partial(update, at) for at in right + left]
        for k, item in enumerate(work_items):
            turn(MIDDLE + k)
            if item is not None:
                pl.when(below)(item)

        @pl.loop(MIDDLE + len(work_items), CHUNKS + LAG + LATE)
        def _(i):
            turn(i)

        w_wait(half // NB)

        @pl.when(below)
        def _():
            panel(width)
            block_row(width)

        log_det()

    @pl.when(even & below)
    def _():
        def arrived(e):
            @pl.loop((e - half) // piece, e // piece)
            def _(i):
                cols_first(1, i).wait_recv()

                @pl.when(c > 0)
                def _():
                    cols_first(0, i).wait_recv()

        arrived(half)
        block_row(half)
        update()
        panel(width)
        arrived(width)
        block_row(width)

    @pl.when(even)
    def _():
        for p in range(steps):
            w_copy(p).wait_send()

        @pl.when(corner)
        def _():
            for k in range(len(tiles)):
                diag_first(k).wait_send()

        @pl.when(below & (c == 0))
        def _():
            for j in range(PANELS):
                own_first(j).wait_send()

        @pl.when(top)
        def _():
            @pl.loop(0, CHUNKS)
            def _(i):
                relay_first(1, i).wait_send()

                @pl.when(c > 0)
                def _():
                    relay_first(0, i).wait_send()

    @pl.when(odd)
    def _():
        for k in range(len(tiles)):
            drain(r >= 0, diag_copies(k))

        @pl.when(below)
        def _():
            @pl.loop(0, PANELS)
            def _(j):
                drain(r >= 0, own_copies(j))

        @pl.loop(0, CHUNKS)
        def _(i):
            @pl.when(top)
            def _():
                cols_first(1, i).wait_send()
                cols_first(0, i).wait_send()

            @pl.when(below)
            def _():
                for n in range(2):
                    drain(r >= 0, cols_copies(n, i))
                drain(r >= 0, relay_copies(1, i))

                @pl.when(c > 1)
                def _():
                    drain(r >= 0, relay_copies(0, i))


def panel_step(mine):
    width = mine.shape[0]
    square = jax.ShapeDtypeStruct((width, width), jnp.float32)
    wide = (width, 2 * width)
    dma = pltpu.SemaphoreType.DMA
    tiles = (width // NB) * (width // NB + 1) // 2 - 1 + STARTS
    return pl.pallas_call(
        panel_kernel,
        out_shape=(
            square, jax.ShapeDtypeStruct(wide, jnp.float32), jax.ShapeDtypeStruct(wide, jnp.float32), square,
            jax.ShapeDtypeStruct((1, NB), jnp.float32),
        ),
        in_specs=[VMEM],
        out_specs=(VMEM,) * 5,
        scratch_shapes=[
            pltpu.VMEM((width, width), jnp.float32), pltpu.VMEM(wide, jnp.float32), pltpu.VMEM(wide, jnp.float32),
            pltpu.VMEM((width, width), jnp.float32), pltpu.VMEM((width, width), jnp.float32),
            pltpu.VMEM((width, width), jnp.float32),
            pltpu.VMEM((NB, NB), jnp.float32), pltpu.VMEM((NB, NB), jnp.float32),
            dma((4, tiles)), dma((tiles,)), dma((2, PANELS)), dma((PANELS,)), dma((4, CHUNKS)), dma((2, CHUNKS)),
            dma((6, CHUNKS)), dma((2, CHUNKS)), dma((width // NB,)), dma((width // NB,)),
        ],
        compiler_params=pltpu.CompilerParams(collective_id=0, has_side_effects=True, vmem_limit_bytes=30 << 20),
    )(mine)


def per_device(mine):
    panel, other, rest, l, logdet = panel_step(mine)
    width = mine.shape[0]
    across = pl.BlockSpec((width, width), lambda s: (0, s))
    whole = pl.BlockSpec((width, width), lambda s: (0, 0))
    block = pl.pallas_call(
        update_kernel,
        grid=(mine.shape[1] // width,),
        out_shape=jax.ShapeDtypeStruct(mine.shape, jnp.float32),
        in_specs=[across, whole, across, whole],
        out_specs=across,
        compiler_params=pltpu.CompilerParams(vmem_limit_bytes=16 << 20),
    )(rest, panel, other, l)
    return block, logdet[0, 0]


def solution(mesh):
    return jax.shard_map(
        per_device, mesh=mesh, in_specs=(P("row", "col"),), out_specs=(P("row", "col"), P()), check_vma=False
    )
```

```python
import functools

import jax
import jax.numpy as jnp
from jax import lax
from jax.experimental import pallas as pl
from jax.experimental.pallas import tpu as pltpu
from jax.sharding import PartitionSpec as P

MESH = pl.DeviceIdType.MESH
NB = 128
BAND = 32
CHUNKS = 32
PANELS = 16
HOPS = 2
FIRST = 2
DELAY = 3
LAST = 5
TURNS = (11, 17, 23, 26, 27, 28, 29)
WAIT = 3
MIDDLE = 22
VMEM = pl.BlockSpec(memory_space=pltpu.VMEM)


def split(a):
    high = a.astype(jnp.bfloat16)
    return high, (a - high.astype(jnp.float32)).astype(jnp.bfloat16)


def dot_split(a, b, axis):
    def dot(u, v):
        return lax.dot_general(u, v, (((1,), (axis,)), ((), ())), preferred_element_type=jnp.float32)

    return dot(a[0], b[0]) + (dot(a[0], b[1]) + dot(a[1], b[0]))


def dot_nt(a, b):
    return dot_split(split(a), split(b), 1)


def dot_nn(a, b):
    return dot_split(split(a), split(b), 0)


def total(terms):
    while len(terms) > 1:
        terms = [a + b for a, b in zip(terms[::2], terms[1::2])]
    return terms[0]


def eliminate(left, right, base):
    sub = lax.broadcasted_iota(jnp.int32, (8, NB), 0)
    left, right = list(left), list(right)
    upper, inverse = [], []

    def row(x, t):
        return jnp.take_along_axis(x, jnp.full((8, NB), t, jnp.int32), axis=0)

    def column(x, t):
        return jnp.broadcast_to(x[:, t : t + 1], (8, NB))

    for p in range(0, len(left), 2):
        first = base + 8 * p
        rest = range(p + 2, len(left))
        cols = [[column(x, first + t) for x in left[p : p + 2]] for t in range(16)]
        mult = {g: [column(left[g], first + t) for t in range(16)] for g in rest}
        v, i = left[p : p + 2], right[p : p + 2]
        u_rows, i_rows, d_rows = list(v), list(i), [None, None]
        for t in range(16):
            at, s = t // 8, t % 8
            here = sub == s
            pivot = row(cols[t][at], s)
            if s:
                u_rows[at] = jnp.where(here, v[at], u_rows[at])
                i_rows[at] = jnp.where(here, i[at], i_rows[at])
                d_rows[at] = jnp.where(here, pivot, d_rows[at])
            else:
                u_rows[at], i_rows[at], d_rows[at] = v[at], i[at], pivot
            recip = 1.0 / pivot
            factor = [x * recip for x in cols[t]]
            factor[at] = jnp.where(here, -recip, factor[at])

            def step(pair):
                taken = row(pair[at], s)
                kept = [jnp.where(here, 0.0, x) if h == at else x for h, x in enumerate(pair)]
                return [x - f * taken for x, f in zip(kept, factor)]

            for w in range(t + 1, 16):
                cols[w] = step(cols[w])
            v, i = step(v), step(i)
        for h in range(2):
            scale = lax.rsqrt(d_rows[h])
            upper.append(u_rows[h] * scale)
            inverse.append(i_rows[h] * scale)
        v_rows = [row(v[t // 8], t % 8) for t in range(16)]
        i_rows = [row(i[t // 8], t % 8) for t in range(16)]
        for g in rest:
            left[g] = left[g] - total([mult[g][t] * v_rows[t] for t in range(16)])
            right[g] = right[g] - total([mult[g][t] * i_rows[t] for t in range(16)])
    return upper, inverse


def factor_block(a):
    lane = lax.broadcasted_iota(jnp.int32, (NB, NB), 1)
    sub = lax.broadcasted_iota(jnp.int32, (NB, NB), 0)
    left, right = a, (lane == sub).astype(jnp.float32)
    upper, inverse = [], []
    for base in range(0, NB, BAND):
        rows = [slice(8 * g, 8 * g + 8) for g in range(BAND // 8)]
        u, i = eliminate([left[x] for x in rows], [right[x] for x in rows], base)
        u, i = jnp.concatenate(u, 0), jnp.concatenate(i, 0)
        upper.append(u)
        inverse.append(i)
        if base + BAND < NB:
            change = dot_nn(u.T[base + BAND :, :], jnp.concatenate([u, i], 1))
            left, right = left[BAND:] - change[:, :NB], right[BAND:] - change[:, NB:]
    upper = jnp.where(lane >= sub, jnp.concatenate(upper, 0), 0.0)
    return upper, jnp.concatenate(inverse, 0)


def factor_all(a_ref, l_ref, w_ref, work, upper, inverse, leave):
    size = w_ref.shape[0]
    work[:NB, :NB] = a_ref[:NB, :NB]
    l_ref[...] = jnp.zeros_like(l_ref)

    @pl.loop(0, size // NB)
    def _(step):
        span = pl.ds(pl.multiple_of(step * NB, NB), NB)
        r, w = factor_block(work[span, span])
        upper[...] = r
        inverse[...] = w
        w_ref[span, span] = inverse[...]
        l_ref[span, span] = upper[...].T
        for p in range(size // NB):

            @pl.when(step == p)
            def _():
                at = slice(p * NB, (p + 1) * NB)
                end = (p + 1) * NB
                if p:
                    leave(p - 1)
                if end < size:
                    below = work[end:, at] if p else a_ref[end:, at]
                    l_ref[end:, at] = dot_nt(below, inverse[...])
                    following = slice(end, end + NB)
                    work[end:, following] = a_ref[end:, following] - dot_nt(l_ref[end:, :end], l_ref[following, :end])
                if p:
                    inner = dot_nn(l_ref[at, : p * NB], w_ref[: p * NB, : p * NB])
                    w_ref[at, : p * NB] = -dot_nn(inverse[...], inner)


def update_kernel(rest_ref, panel_ref, other_ref, l_ref, out_ref):
    r, c = lax.axis_index("row"), lax.axis_index("col")
    leading = (c == 0) & (pl.program_id(0) == 0)

    @pl.when(r == 0)
    def _():
        out_ref[...] = jnp.where(leading, l_ref[...], 0.0)

    @pl.when((r > 0) & leading)
    def _():
        out_ref[...] = panel_ref[...]

    @pl.when((r > 0) & jnp.logical_not(leading))
    def _():
        half = panel_ref.shape[1] // 2
        out_ref[...] = rest_ref[...] - dot_nn(panel_ref[:, half:], other_ref[half:, :])


def panel_kernel(mine_ref, panel_ref, other_ref, rest_ref, l_ref, logdet_ref,
                 own_ref, cols_ref, w_ref, work, upper, inverse,
                 own_send, own_recv, cols_send, cols_recv, w_send, w_recv):
    rows, columns = lax.axis_size("row"), lax.axis_size("col")
    r, c = lax.axis_index("row"), lax.axis_index("col")
    q, x = r // 2, r % 2
    other = r + 1 - 2 * x
    partner = c + 1 - 2 * (c % 2)
    odd = c % 2 == 1
    even = jnp.logical_not(odd)
    width = own_ref.shape[0]
    top = r == 0
    below = jnp.logical_not(top)
    corner = top & (c == 0)

    links = [
        ((r, partner), partner >= 0), ((other, c), other >= 0),
        ((r - 2, c), r >= 2), ((r + 2, c), r + 2 < rows),
        ((r, c - 2), c >= 2), ((r, c + 2), c + 2 < columns),
    ]
    barrier = pltpu.get_barrier_semaphore()
    for device, exists in links:
        @pl.when(exists)
        def _():
            pl.semaphore_signal(barrier, inc=1, device_id=device, device_id_type=MESH)
    peers = sum(jnp.where(exists, 1, 0).astype(jnp.int32) for _, exists in links)
    pl.semaphore_wait(barrier, peers)

    def send(source, target, send_sem, recv_sem, device):
        return pltpu.make_async_remote_copy(
            src_ref=source, dst_ref=target, send_sem=send_sem, recv_sem=recv_sem,
            device_id=device, device_id_type=MESH,
        )

    def start(condition, copies):
        for exists, copy in copies:
            @pl.when(condition & exists)
            def _():
                copy.start()

    def drain(condition, copies):
        for exists, copy in copies:
            @pl.when(condition & exists)
            def _():
                copy.wait_send()

    side_row = jnp.where(x == 0, r + 1, r - 2)
    has_side = ((x == 0) & (q >= 1)) | (r == 3)

    steps = width // NB
    pieces = [(pl.ds(p * NB, NB), pl.ds(0, (p + 1) * NB)) for p in range(steps - 1)]
    pieces += [(pl.ds((steps - 1) * NB, NB), pl.ds(j * NB, NB)) for j in range(steps)]

    def w_first(m):
        part = w_ref.at[pieces[m]]
        return send(part, part, w_send.at[0, m], w_recv.at[m], (r, c + 1))

    def w_copies(m):
        part = w_ref.at[pieces[m]]

        def to(n, device):
            return send(part, part, w_send.at[n, m], w_recv.at[m], device)

        return [
            ((c == 1) & (x == 0) & (r + 2 < rows), to(0, (r + 2, c))),
            ((c == 1) & has_side, to(1, (side_row, c))),
            (c + 2 < columns, to(2, (r, c + 2))),
            (jnp.logical_not(top & (c == 1)), to(3, (r, c - 1))),
        ]

    def w_relay(m):
        copies = w_copies(m)
        copies[0][1].wait_recv()
        start(r >= 0, copies)

    deep = width // PANELS

    def own_part(j):
        return own_ref.at[pl.ds(pl.multiple_of(j * deep, deep), deep), :]

    def own_source(j):
        return mine_ref.at[pl.ds(pl.multiple_of(j * deep, deep), deep), pl.ds(0, width)]

    def own_load(j):
        return pltpu.make_async_copy(own_source(j), own_part(j), own_recv.at[j])

    def own_copies(j, source):
        def to(n, device):
            return send(source, own_part(j), own_send.at[n, j], own_recv.at[j], device)

        return [(c + 2 < columns, to(0, (r, c + 2))), (c >= 0, to(1, (r, c + 1)))]

    def own_wait(j):
        own_copies(j, own_part(j))[0][1].wait_recv()

    piece = width // CHUNKS

    def cols_part(ref, n, i):
        return ref.at[pl.ds(i * piece, piece), pl.ds(n * width, width)]

    def cols_copies(n, i, source):
        def to(m, device):
            return send(source, cols_part(cols_ref, n, i), cols_send.at[2 * n + m, i], cols_recv.at[n, i], device)

        return [((x == n) & (r + 2 < rows), to(0, (r + 2, c))), ((x == n) & (q >= 1) | (r == 3) & (n == 0), to(1, (sides[n], c)))]

    sides = [side_row, r - 1]
    relays = [(c > 0) & (((x == 0) & (q >= 1)) | (r == 3)), x == 1]

    def cols_first(n, i):
        source = cols_part(mine_ref, n, i)
        return send(source, cols_part(cols_ref, n, i), cols_send.at[2 * n, i], cols_recv.at[n, i], (r + 2 - n, c))

    def cols_wait(n, i):
        cols_first(n, i).wait_recv()

    def arrived(e):
        for n in range(2):
            @pl.when(jnp.logical_not(relays[n]) & ((c > 0) | (n == 1)))
            def _():
                for i in range((e - half) // piece, e // piece):
                    cols_wait(n, i)

    half = width // 2

    def log_det():
        here = lax.broadcasted_iota(jnp.int32, (NB, NB), 0) == lax.broadcasted_iota(jnp.int32, (NB, NB), 1)
        blocks = [slice(p * NB, (p + 1) * NB) for p in range(steps)]
        logs = sum(jnp.log(jnp.where(here, w_ref[at, at], 1.0)) for at in blocks)
        across = jnp.sum(logs, axis=0, keepdims=True)
        logdet_ref[...] = jnp.broadcast_to(-2.0 * jnp.sum(across, axis=1, keepdims=True), logdet_ref.shape)

    def panel(e, at=slice(None)):
        own = split(own_ref[at, :e])
        panel_ref[at, e - half : e] = dot_split(own, split(w_ref[e - half : e, :e]), 1)

    def block_row(e, at=slice(None)):
        other_ref[e - half : e, at] = dot_split(split(w_ref[e - half : e, :e]), split(cols_ref[:e, at]), 0)

    def update(at=slice(None)):
        rest_ref[:, at] = mine_ref[:, at] - dot_nn(panel_ref[:, :half], other_ref[:half, at])

    for p in range(steps):
        if p * NB % half == 0 and half > NB:
            w_ref[p * NB : (p + 1) * NB, (p + 1) * NB : p * NB + half] = jnp.zeros((NB, half - NB), jnp.float32)

    @pl.when(top)
    def _():
        for i in range(CHUNKS):
            cols_first(1, i).start()

            @pl.when(c > 0)
            def _():
                cols_first(0, i).start()

    @pl.when(below & (c == 0))
    def _():
        for j in range(PANELS):
            start(c >= 0, own_copies(j, own_source(j)))
        for j in range(PANELS):
            own_load(j).start()

    @pl.when(corner)
    def _():
        factor_all(mine_ref, l_ref, w_ref, work, upper, inverse, lambda p: w_first(p).start())
        log_det()
        for m in range(steps - 1, len(pieces)):
            w_first(m).start()

    @pl.when(top & odd)
    def _():
        for m in range(len(pieces)):
            w_relay(m)

    @pl.when(top & even & (c > 0))
    def _():
        for m in range(len(pieces)):
            w_first(m).wait_recv()

    first_half = half // NB
    patient = r == 1

    def w_arrive(first, last):
        @pl.when(even)
        def _():
            for m in range(first, last):
                w_first(m).wait_recv()

    def panel_arrive():
        @pl.when(c == 0)
        def _():
            for j in range(PANELS):
                own_load(j).wait()

        @pl.when(odd)
        def _():
            for j in range(PANELS):
                own_wait(j)

    lower = [slice(i, i + half) for i in range(0, 2 * width, half)]
    rows_of, right = lower[: width // half], lower[width // half :]
    items = [functools.partial(block_row, half, at) for at in right + rows_of]
    items += [functools.partial(panel, half, at) for at in rows_of]
    items += [functools.partial(update, at) for at in right + rows_of]

    @pl.when(below)
    def _():
        for i in range(CHUNKS):
            for n in range(2):
                @pl.when(relays[n])
                def _():
                    cols_wait(n, i)
                    start(c >= 0, cols_copies(n, i, cols_part(cols_ref, n, i)))

            for hop in range(1, HOPS + 1):
                j = i - min(FIRST + DELAY * (hop - 1), LAST)
                if 0 <= j < PANELS:
                    @pl.when(even & (c == 2 * hop if hop < HOPS else c >= 2 * hop))
                    def _():
                        own_wait(j)
                        start(c >= 0, own_copies(j, own_part(j)))

            for m, turn in enumerate(TURNS):
                for late, plane in ((0, c == 1), (WAIT, c > 1)):
                    if min(turn + late, CHUNKS - 1) == i:
                        @pl.when(odd & plane & jnp.logical_not(patient))
                        def _():
                            w_relay(m)

            if i == MIDDLE:
                @pl.when(jnp.logical_not(patient))
                def _():
                    w_arrive(0, first_half)
                    panel_arrive()
                    arrived(half)

            if MIDDLE <= i < MIDDLE + len(items):
                pl.when(jnp.logical_not(patient))(items[i - MIDDLE])

        @pl.when(patient)
        def _():
            @pl.when(odd)
            def _():
                for m in range(len(pieces)):
                    w_relay(m)

            w_arrive(0, first_half)
            panel_arrive()
            arrived(half)
            block_row(half)
            panel(half)
            update()

        w_arrive(first_half, len(pieces))
        panel(width)
        arrived(width)
        block_row(width)

    @pl.when(jnp.logical_not(corner))
    def _():
        log_det()

    @pl.when(corner)
    def _():
        for m in range(len(pieces)):
            w_first(m).wait_send()

    for m in range(len(pieces)):
        drain(odd, w_copies(m))

    @pl.when(below & even)
    def _():
        for j in range(PANELS):
            drain(c >= 0, own_copies(j, own_part(j)))

    for i in range(CHUNKS):
        @pl.when(top)
        def _():
            cols_first(1, i).wait_send()

            @pl.when(c > 0)
            def _():
                cols_first(0, i).wait_send()

        for n in range(2):
            drain(below & relays[n], cols_copies(n, i, cols_part(cols_ref, n, i)))


def panel_step(mine):
    width = mine.shape[0]
    square = jax.ShapeDtypeStruct((width, width), jnp.float32)
    wide = (width, 2 * width)
    dma = pltpu.SemaphoreType.DMA
    pieces = 2 * (width // NB) - 1
    return pl.pallas_call(
        panel_kernel,
        out_shape=(
            square, jax.ShapeDtypeStruct(wide, jnp.float32), jax.ShapeDtypeStruct(wide, jnp.float32), square,
            jax.ShapeDtypeStruct((1, NB), jnp.float32),
        ),
        in_specs=[VMEM],
        out_specs=(VMEM,) * 5,
        scratch_shapes=[
            pltpu.VMEM((width, width), jnp.float32), pltpu.VMEM(wide, jnp.float32),
            pltpu.VMEM((width, width), jnp.float32), pltpu.VMEM((width, width), jnp.float32),
            pltpu.VMEM((NB, NB), jnp.float32), pltpu.VMEM((NB, NB), jnp.float32),
            dma((2, PANELS)), dma((PANELS,)), dma((4, CHUNKS)), dma((2, CHUNKS)), dma((4, pieces)), dma((pieces,)),
        ],
        compiler_params=pltpu.CompilerParams(collective_id=0, has_side_effects=True, vmem_limit_bytes=30 << 20),
    )(mine)


def per_device(mine):
    panel, other, rest, l, logdet = panel_step(mine)
    width = mine.shape[0]
    across = pl.BlockSpec((width, width), lambda s: (0, s))
    whole = pl.BlockSpec((width, width), lambda s: (0, 0))
    block = pl.pallas_call(
        update_kernel,
        grid=(mine.shape[1] // width,),
        out_shape=jax.ShapeDtypeStruct(mine.shape, jnp.float32),
        in_specs=[across, whole, across, whole],
        out_specs=across,
        compiler_params=pltpu.CompilerParams(vmem_limit_bytes=16 << 20),
    )(rest, panel, other, l)
    return block, logdet[0, 0]


def solution(mesh):
    return jax.shard_map(
        per_device, mesh=mesh, in_specs=(P("row", "col"),), out_specs=(P("row", "col"), P()), check_vma=False
    )
```

```python
import functools

import jax
import jax.numpy as jnp
from jax import lax
from jax.experimental import pallas as pl
from jax.experimental.pallas import tpu as pltpu
from jax.sharding import PartitionSpec as P

MESH = pl.DeviceIdType.MESH
NB = 128
BAND = 32
CHUNKS = 32
PANELS = 16
HOPS = 2
FIRST = 2
DELAY = 3
LAST = 5
TURNS = (11, 17, 23, 26, 27, 28, 29)
WAIT = 3
MIDDLE = 22
VMEM = pl.BlockSpec(memory_space=pltpu.VMEM)


def split(a):
    high = a.astype(jnp.bfloat16)
    return high, (a - high.astype(jnp.float32)).astype(jnp.bfloat16)


def dot_split(a, b, axis):
    def dot(u, v):
        return lax.dot_general(u, v, (((1,), (axis,)), ((), ())), preferred_element_type=jnp.float32)

    return dot(a[0], b[0]) + (dot(a[0], b[1]) + dot(a[1], b[0]))


def dot_nt(a, b):
    return dot_split(split(a), split(b), 1)


def dot_nn(a, b):
    return dot_split(split(a), split(b), 0)


def total(terms):
    while len(terms) > 1:
        terms = [a + b for a, b in zip(terms[::2], terms[1::2])]
    return terms[0]


def eliminate(left, right, base):
    sub = lax.broadcasted_iota(jnp.int32, (8, NB), 0)
    left, right = list(left), list(right)
    upper, inverse = [], []

    def row(x, t):
        return jnp.take_along_axis(x, jnp.full((8, NB), t, jnp.int32), axis=0)

    def column(x, t):
        return jnp.broadcast_to(x[:, t : t + 1], (8, NB))

    for p in range(0, len(left), 2):
        first = base + 8 * p
        rest = range(p + 2, len(left))
        cols = [[column(x, first + t) for x in left[p : p + 2]] for t in range(16)]
        mult = {g: [column(left[g], first + t) for t in range(16)] for g in rest}
        v, i = left[p : p + 2], right[p : p + 2]
        u_rows, i_rows, d_rows = list(v), list(i), [None, None]
        for t in range(16):
            at, s = t // 8, t % 8
            here = sub == s
            pivot = row(cols[t][at], s)
            if s:
                u_rows[at] = jnp.where(here, v[at], u_rows[at])
                i_rows[at] = jnp.where(here, i[at], i_rows[at])
                d_rows[at] = jnp.where(here, pivot, d_rows[at])
            else:
                u_rows[at], i_rows[at], d_rows[at] = v[at], i[at], pivot
            recip = 1.0 / pivot
            factor = [x * recip for x in cols[t]]
            factor[at] = jnp.where(here, -recip, factor[at])

            def step(pair):
                taken = row(pair[at], s)
                kept = [jnp.where(here, 0.0, x) if h == at else x for h, x in enumerate(pair)]
                return [x - f * taken for x, f in zip(kept, factor)]

            for w in range(t + 1, 16):
                cols[w] = step(cols[w])
            v, i = step(v), step(i)
        for h in range(2):
            scale = lax.rsqrt(d_rows[h])
            upper.append(u_rows[h] * scale)
            inverse.append(i_rows[h] * scale)
        v_rows = [row(v[t // 8], t % 8) for t in range(16)]
        i_rows = [row(i[t // 8], t % 8) for t in range(16)]
        for g in rest:
            left[g] = left[g] - total([mult[g][t] * v_rows[t] for t in range(16)])
            right[g] = right[g] - total([mult[g][t] * i_rows[t] for t in range(16)])
    return upper, inverse


def factor_block(a):
    lane = lax.broadcasted_iota(jnp.int32, (NB, NB), 1)
    sub = lax.broadcasted_iota(jnp.int32, (NB, NB), 0)
    left, right = a, (lane == sub).astype(jnp.float32)
    upper, inverse = [], []
    for base in range(0, NB, BAND):
        rows = [slice(8 * g, 8 * g + 8) for g in range(BAND // 8)]
        u, i = eliminate([left[x] for x in rows], [right[x] for x in rows], base)
        u, i = jnp.concatenate(u, 0), jnp.concatenate(i, 0)
        upper.append(u)
        inverse.append(i)
        if base + BAND < NB:
            change = dot_nn(u.T[base + BAND :, :], jnp.concatenate([u, i], 1))
            left, right = left[BAND:] - change[:, :NB], right[BAND:] - change[:, NB:]
    upper = jnp.where(lane >= sub, jnp.concatenate(upper, 0), 0.0)
    return upper, jnp.concatenate(inverse, 0)


def factor_all(a_ref, l_ref, w_ref, work, upper, inverse, leave):
    size = w_ref.shape[0]
    work[:NB, :NB] = a_ref[:NB, :NB]
    l_ref[...] = jnp.zeros_like(l_ref)

    @pl.loop(0, size // NB)
    def _(step):
        span = pl.ds(pl.multiple_of(step * NB, NB), NB)
        r, w = factor_block(work[span, span])
        upper[...] = r
        inverse[...] = w
        w_ref[span, span] = inverse[...]
        l_ref[span, span] = upper[...].T
        for p in range(size // NB):

            @pl.when(step == p)
            def _():
                at = slice(p * NB, (p + 1) * NB)
                end = (p + 1) * NB
                if p:
                    leave(p - 1)
                if end < size:
                    below = work[end:, at] if p else a_ref[end:, at]
                    l_ref[end:, at] = dot_nt(below, inverse[...])
                    following = slice(end, end + NB)
                    work[end:, following] = a_ref[end:, following] - dot_nt(l_ref[end:, :end], l_ref[following, :end])
                if p:
                    inner = dot_nn(l_ref[at, : p * NB], w_ref[: p * NB, : p * NB])
                    w_ref[at, : p * NB] = -dot_nn(inverse[...], inner)


def update_kernel(rest_ref, panel_ref, other_ref, l_ref, out_ref):
    r, c = lax.axis_index("row"), lax.axis_index("col")
    leading = (c == 0) & (pl.program_id(0) == 0)

    @pl.when(r == 0)
    def _():
        out_ref[...] = jnp.where(leading, l_ref[...], 0.0)

    @pl.when((r > 0) & leading)
    def _():
        out_ref[...] = panel_ref[...]

    @pl.when((r > 0) & jnp.logical_not(leading))
    def _():
        half = panel_ref.shape[1] // 2
        out_ref[...] = rest_ref[...] - dot_nn(panel_ref[:, half:], other_ref[half:, :])


def panel_kernel(mine_ref, panel_ref, other_ref, rest_ref, l_ref, logdet_ref,
                 own_ref, cols_ref, w_ref, work, upper, inverse,
                 own_send, own_recv, cols_send, cols_recv, w_send, w_recv):
    rows, columns = lax.axis_size("row"), lax.axis_size("col")
    r, c = lax.axis_index("row"), lax.axis_index("col")
    q, x = r // 2, r % 2
    other = r + 1 - 2 * x
    partner = c + 1 - 2 * (c % 2)
    odd = c % 2 == 1
    even = jnp.logical_not(odd)
    width = own_ref.shape[0]
    top = r == 0
    below = jnp.logical_not(top)
    corner = top & (c == 0)

    links = [
        ((r, partner), partner >= 0), ((other, c), other >= 0),
        ((r - 2, c), r >= 2), ((r + 2, c), r + 2 < rows),
        ((r, c - 2), c >= 2), ((r, c + 2), c + 2 < columns),
    ]
    barrier = pltpu.get_barrier_semaphore()
    for device, exists in links:
        @pl.when(exists)
        def _():
            pl.semaphore_signal(barrier, inc=1, device_id=device, device_id_type=MESH)
    peers = sum(jnp.where(exists, 1, 0).astype(jnp.int32) for _, exists in links)
    pl.semaphore_wait(barrier, peers)

    def send(source, target, send_sem, recv_sem, device):
        return pltpu.make_async_remote_copy(
            src_ref=source, dst_ref=target, send_sem=send_sem, recv_sem=recv_sem,
            device_id=device, device_id_type=MESH,
        )

    def start(condition, copies):
        for exists, copy in copies:
            @pl.when(condition & exists)
            def _():
                copy.start()

    side_row = jnp.where(x == 0, r + 1, r - 2)
    has_side = ((x == 0) & (q >= 1)) | (r == 3)

    steps = width // NB
    pieces = [(pl.ds(p * NB, NB), pl.ds(0, (p + 1) * NB)) for p in range(steps - 1)]
    pieces += [(pl.ds((steps - 1) * NB, NB), pl.ds(j * NB, NB)) for j in range(steps)]

    def w_first(m):
        part = w_ref.at[pieces[m]]
        return send(part, part, w_send.at[0], w_recv.at[m], (r, c + 1))

    def w_copies(m):
        part = w_ref.at[pieces[m]]

        def to(n, device):
            return send(part, part, w_send.at[n], w_recv.at[m], device)

        return [
            ((c == 1) & (x == 0) & (r + 2 < rows), to(0, (r + 2, c))),
            ((c == 1) & has_side, to(1, (side_row, c))),
            (c + 2 < columns, to(2, (r, c + 2))),
            (jnp.logical_not(top & (c == 1)), to(3, (r, c - 1))),
        ]

    def w_relay(m):
        copies = w_copies(m)
        copies[0][1].wait_recv()
        start(r >= 0, copies)

    deep = width // PANELS

    def own_part(j):
        return own_ref.at[pl.ds(pl.multiple_of(j * deep, deep), deep), :]

    def own_source(j):
        return mine_ref.at[pl.ds(pl.multiple_of(j * deep, deep), deep), pl.ds(0, width)]

    def own_load(j):
        return pltpu.make_async_copy(own_source(j), own_part(j), own_recv.at[j])

    def own_copies(j, source):
        def to(n, device):
            return send(source, own_part(j), own_send.at[n], own_recv.at[j], device)

        return [(c + 2 < columns, to(0, (r, c + 2))), (c >= 0, to(1, (r, c + 1)))]

    def own_wait(j):
        own_copies(j, own_part(j))[0][1].wait_recv()

    piece = width // CHUNKS

    def cols_part(ref, n, i):
        return ref.at[pl.ds(i * piece, piece), pl.ds(n * width, width)]

    def cols_copies(n, i, source):
        def to(m, device):
            return send(source, cols_part(cols_ref, n, i), cols_send.at[2 * n + m], cols_recv.at[n, i], device)

        return [((x == n) & (r + 2 < rows), to(0, (r + 2, c))), ((x == n) & (q >= 1) | (r == 3) & (n == 0), to(1, (sides[n], c)))]

    sides = [side_row, r - 1]
    relays = [(c > 0) & (((x == 0) & (q >= 1)) | (r == 3)), x == 1]

    def cols_first(n, i):
        source = cols_part(mine_ref, n, i)
        return send(source, cols_part(cols_ref, n, i), cols_send.at[2 * n], cols_recv.at[n, i], (r + 2 - n, c))

    def cols_wait(n, i):
        cols_first(n, i).wait_recv()

    def arrived(e):
        for n in range(2):
            @pl.when(jnp.logical_not(relays[n]) & ((c > 0) | (n == 1)))
            def _():
                for i in range((e - half) // piece, e // piece):
                    cols_wait(n, i)

    half = width // 2

    def log_det():
        here = lax.broadcasted_iota(jnp.int32, (NB, NB), 0) == lax.broadcasted_iota(jnp.int32, (NB, NB), 1)
        blocks = [slice(p * NB, (p + 1) * NB) for p in range(steps)]
        logs = sum(jnp.log(jnp.where(here, w_ref[at, at], 1.0)) for at in blocks)
        across = jnp.sum(logs, axis=0, keepdims=True)
        logdet_ref[...] = jnp.broadcast_to(-2.0 * jnp.sum(across, axis=1, keepdims=True), logdet_ref.shape)

    def panel(e, at=slice(None)):
        own = split(own_ref[at, :e])
        panel_ref[at, e - half : e] = dot_split(own, split(w_ref[e - half : e, :e]), 1)

    def block_row(e, at=slice(None)):
        other_ref[e - half : e, at] = dot_split(split(w_ref[e - half : e, :e]), split(cols_ref[:e, at]), 0)

    def update(at=slice(None)):
        rest_ref[:, at] = mine_ref[:, at] - dot_nn(panel_ref[:, :half], other_ref[:half, at])

    for p in range(steps):
        if p * NB % half == 0 and half > NB:
            w_ref[p * NB : (p + 1) * NB, (p + 1) * NB : p * NB + half] = jnp.zeros((NB, half - NB), jnp.float32)

    @pl.when(top)
    def _():
        for i in range(CHUNKS):
            cols_first(1, i).start()

            @pl.when(c > 0)
            def _():
                cols_first(0, i).start()

    @pl.when(below & (c == 0))
    def _():
        for j in range(PANELS):
            start(c >= 0, own_copies(j, own_source(j)))
        for j in range(PANELS):
            own_load(j).start()

    @pl.when(corner)
    def _():
        factor_all(mine_ref, l_ref, w_ref, work, upper, inverse, lambda p: w_first(p).start())
        log_det()
        for m in range(steps - 1, len(pieces)):
            w_first(m).start()

    @pl.when(top & odd)
    def _():
        for m in range(len(pieces)):
            w_relay(m)

    @pl.when(top & even & (c > 0))
    def _():
        for m in range(len(pieces)):
            w_first(m).wait_recv()

    first_half = half // NB
    patient = r == 1
    between = (x == 1) & (r + 2 >= rows)

    def w_arrive(first, last):
        @pl.when(even)
        def _():
            for m in range(first, last):
                w_first(m).wait_recv()

    def panel_arrive():
        @pl.when(c == 0)
        def _():
            for j in range(PANELS):
                own_load(j).wait()

        @pl.when(odd)
        def _():
            for j in range(PANELS):
                own_wait(j)

    lower = [slice(i, i + half) for i in range(0, 2 * width, half)]
    rows_of, right = lower[: width // half], lower[width // half :]
    items = [functools.partial(block_row, half, at) for at in right + rows_of]
    items += [functools.partial(panel, half, at) for at in rows_of]
    items += [functools.partial(update, at) for at in right + rows_of]

    @pl.when(below)
    def _():
        for i in range(CHUNKS):
            for n in range(2):
                @pl.when(relays[n])
                def _():
                    cols_wait(n, i)
                    start(c >= 0, cols_copies(n, i, cols_part(cols_ref, n, i)))

            for hop in range(1, HOPS + 1):
                j = i - min(FIRST + DELAY * (hop - 1), LAST)
                if 0 <= j < PANELS:
                    @pl.when(even & (c == 2 * hop if hop < HOPS else c >= 2 * hop))
                    def _():
                        own_wait(j)
                        start(c >= 0, own_copies(j, own_part(j)))

            for m, turn in enumerate(TURNS):
                for late, plane in ((0, c == 1), (WAIT, c > 1)):
                    if min(turn + late, CHUNKS - 1) == i:
                        @pl.when(odd & plane & jnp.logical_not(patient))
                        def _():
                            w_relay(m)

            if i == MIDDLE:
                @pl.when(between)
                def _():
                    w_arrive(0, first_half)
                    panel_arrive()
                    arrived(half)

            if MIDDLE <= i < MIDDLE + len(items):
                pl.when(between)(items[i - MIDDLE])

        @pl.when(patient & odd)
        def _():
            for m in range(len(pieces)):
                w_relay(m)

        @pl.when(jnp.logical_not(between))
        def _():
            w_arrive(0, first_half)
            panel_arrive()
            arrived(half)
            block_row(half)
            panel(half)
            update()

        w_arrive(first_half, len(pieces))
        panel(width)
        arrived(width)
        block_row(width)

    @pl.when(jnp.logical_not(corner))
    def _():
        log_det()

    def sent(condition, part, sem):
        @pl.when(condition)
        def _():
            send(part, part, sem, w_recv.at[0], (r, partner)).wait_send()

    inverse_part = cols_ref.at[pl.ds(0, (steps + 1) * NB // 4), :]
    sent(corner, inverse_part, w_send.at[0])
    for n, (exists, _) in enumerate(w_copies(0)):
        sent(odd & exists, inverse_part, w_send.at[n])
    for n, (exists, _) in enumerate(own_copies(0, own_part(0))):
        sent(below & even & exists, own_ref, own_send.at[n])
    for n in range(2):
        part = cols_ref.at[:, pl.ds(n * width, width)]
        sent(top & ((c > 0) | (n == 1)), part, cols_send.at[2 * n])
        for m, (exists, _) in enumerate(cols_copies(n, 0, cols_part(cols_ref, n, 0))):
            sent(below & relays[n] & exists, part, cols_send.at[2 * n + m])


def panel_step(mine):
    width = mine.shape[0]
    square = jax.ShapeDtypeStruct((width, width), jnp.float32)
    wide = (width, 2 * width)
    dma = pltpu.SemaphoreType.DMA
    pieces = 2 * (width // NB) - 1
    return pl.pallas_call(
        panel_kernel,
        out_shape=(
            square, jax.ShapeDtypeStruct(wide, jnp.float32), jax.ShapeDtypeStruct(wide, jnp.float32), square,
            jax.ShapeDtypeStruct((1, NB), jnp.float32),
        ),
        in_specs=[VMEM],
        out_specs=(VMEM,) * 5,
        scratch_shapes=[
            pltpu.VMEM((width, width), jnp.float32), pltpu.VMEM(wide, jnp.float32),
            pltpu.VMEM((width, width), jnp.float32), pltpu.VMEM((width, width), jnp.float32),
            pltpu.VMEM((NB, NB), jnp.float32), pltpu.VMEM((NB, NB), jnp.float32),
            dma((2,)), dma((PANELS,)), dma((4,)), dma((2, CHUNKS)), dma((4,)), dma((pieces,)),
        ],
        compiler_params=pltpu.CompilerParams(collective_id=0, has_side_effects=True, vmem_limit_bytes=30 << 20),
    )(mine)


def per_device(mine):
    panel, other, rest, l, logdet = panel_step(mine)
    width = mine.shape[0]
    across = pl.BlockSpec((width, width), lambda s: (0, s))
    whole = pl.BlockSpec((width, width), lambda s: (0, 0))
    block = pl.pallas_call(
        update_kernel,
        grid=(mine.shape[1] // width,),
        out_shape=jax.ShapeDtypeStruct(mine.shape, jnp.float32),
        in_specs=[across, whole, across, whole],
        out_specs=across,
        compiler_params=pltpu.CompilerParams(vmem_limit_bytes=16 << 20),
    )(rest, panel, other, l)
    return block, logdet[0, 0]


def solution(mesh):
    return jax.shard_map(
        per_device, mesh=mesh, in_specs=(P("row", "col"),), out_specs=(P("row", "col"), P()), check_vma=False
    )
```

```python
import functools

import jax
import jax.numpy as jnp
from jax import lax
from jax.experimental import pallas as pl
from jax.experimental.pallas import tpu as pltpu
from jax.sharding import PartitionSpec as P

MESH = pl.DeviceIdType.MESH
NB = 128
BAND = 32
CHUNKS = 32
PANELS = 16
HOPS = 2
FIRST = 2
DELAY = 3
LAST = 5
TURNS = (10, 11, 15, 16, 17, 18, 21, 21, 22, 22, 23, 24, 24, 25, 25, 26, 26, 27, 27, 28)
FOLLOW = 12
WAIT = 3
MIDDLE = 22
VMEM = pl.BlockSpec(memory_space=pltpu.VMEM)


def split(a):
    high = a.astype(jnp.bfloat16)
    return high, (a - high.astype(jnp.float32)).astype(jnp.bfloat16)


def dot_split(a, b, axis):
    def dot(u, v):
        return lax.dot_general(u, v, (((1,), (axis,)), ((), ())), preferred_element_type=jnp.float32)

    return dot(a[0], b[0]) + (dot(a[0], b[1]) + dot(a[1], b[0]))


def dot_nt(a, b):
    return dot_split(split(a), split(b), 1)


def dot_nn(a, b):
    return dot_split(split(a), split(b), 0)


def total(terms):
    while len(terms) > 1:
        terms = [a + b for a, b in zip(terms[::2], terms[1::2])]
    return terms[0]


def eliminate(left, right, base):
    sub = lax.broadcasted_iota(jnp.int32, (8, NB), 0)
    left, right = list(left), list(right)
    upper, inverse = [], []

    def row(x, t):
        return jnp.take_along_axis(x, jnp.full((8, NB), t, jnp.int32), axis=0)

    def column(x, t):
        return jnp.broadcast_to(x[:, t : t + 1], (8, NB))

    for p in range(0, len(left), 2):
        first = base + 8 * p
        rest = range(p + 2, len(left))
        cols = [[column(x, first + t) for x in left[p : p + 2]] for t in range(16)]
        mult = {g: [column(left[g], first + t) for t in range(16)] for g in rest}
        v, i = left[p : p + 2], right[p : p + 2]
        u_rows, i_rows, d_rows = list(v), list(i), [None, None]
        for t in range(16):
            at, s = t // 8, t % 8
            here = sub == s
            pivot = row(cols[t][at], s)
            if s:
                u_rows[at] = jnp.where(here, v[at], u_rows[at])
                i_rows[at] = jnp.where(here, i[at], i_rows[at])
                d_rows[at] = jnp.where(here, pivot, d_rows[at])
            else:
                u_rows[at], i_rows[at], d_rows[at] = v[at], i[at], pivot
            recip = 1.0 / pivot
            factor = [x * recip for x in cols[t]]
            factor[at] = jnp.where(here, -recip, factor[at])

            def step(pair):
                taken = row(pair[at], s)
                kept = [jnp.where(here, 0.0, x) if h == at else x for h, x in enumerate(pair)]
                return [x - f * taken for x, f in zip(kept, factor)]

            for w in range(t + 1, 16):
                cols[w] = step(cols[w])
            v, i = step(v), step(i)
        for h in range(2):
            scale = lax.rsqrt(d_rows[h])
            upper.append(u_rows[h] * scale)
            inverse.append(i_rows[h] * scale)
        v_rows = [row(v[t // 8], t % 8) for t in range(16)]
        i_rows = [row(i[t // 8], t % 8) for t in range(16)]
        for g in rest:
            left[g] = left[g] - total([mult[g][t] * v_rows[t] for t in range(16)])
            right[g] = right[g] - total([mult[g][t] * i_rows[t] for t in range(16)])
    return upper, inverse


def factor_block(a):
    lane = lax.broadcasted_iota(jnp.int32, (NB, NB), 1)
    sub = lax.broadcasted_iota(jnp.int32, (NB, NB), 0)
    left, right = a, (lane == sub).astype(jnp.float32)
    upper, inverse = [], []
    for base in range(0, NB, BAND):
        rows = [slice(8 * g, 8 * g + 8) for g in range(BAND // 8)]
        u, i = eliminate([left[x] for x in rows], [right[x] for x in rows], base)
        u, i = jnp.concatenate(u, 0), jnp.concatenate(i, 0)
        upper.append(u)
        inverse.append(i)
        if base + BAND < NB:
            change = dot_nn(u.T[base + BAND :, :], jnp.concatenate([u, i], 1))
            left, right = left[BAND:] - change[:, :NB], right[BAND:] - change[:, NB:]
    upper = jnp.where(lane >= sub, jnp.concatenate(upper, 0), 0.0)
    return upper, jnp.concatenate(inverse, 0)


def factor_all(a_ref, l_ref, w_ref, work, upper, inverse, leave):
    size = w_ref.shape[0]
    work[:NB, :NB] = a_ref[:NB, :NB]
    l_ref[...] = jnp.zeros_like(l_ref)

    @pl.loop(0, size // NB)
    def _(step):
        span = pl.ds(pl.multiple_of(step * NB, NB), NB)
        r, w = factor_block(work[span, span])
        upper[...] = r
        inverse[...] = w
        w_ref[span, span] = inverse[...]
        l_ref[span, span] = upper[...].T
        for p in range(size // NB):

            @pl.when(step == p)
            def _():
                at = slice(p * NB, (p + 1) * NB)
                end = (p + 1) * NB
                if p:
                    leave(p - 1)
                if end < size:
                    below = work[end:, at] if p else a_ref[end:, at]
                    l_ref[end:, at] = dot_nt(below, inverse[...])
                    following = slice(end, end + NB)
                    work[end:, following] = a_ref[end:, following] - dot_nt(l_ref[end:, :end], l_ref[following, :end])
                if p:
                    inner = dot_nn(l_ref[at, : p * NB], w_ref[: p * NB, : p * NB])
                    w_ref[at, : p * NB] = -dot_nn(inverse[...], inner)


def update_kernel(rest_ref, panel_ref, other_ref, l_ref, out_ref):
    r, c = lax.axis_index("row"), lax.axis_index("col")
    leading = (c == 0) & (pl.program_id(0) == 0)

    @pl.when(r == 0)
    def _():
        out_ref[...] = jnp.where(leading, l_ref[...], 0.0)

    @pl.when((r > 0) & leading)
    def _():
        out_ref[...] = panel_ref[...]

    @pl.when((r > 0) & jnp.logical_not(leading))
    def _():
        half = panel_ref.shape[1] // 2
        out_ref[...] = rest_ref[...] - dot_nn(panel_ref[:, half:], other_ref[half:, :])


def panel_kernel(mine_ref, panel_ref, other_ref, rest_ref, l_ref, logdet_ref,
                 own_ref, cols_ref, w_ref, work, upper, inverse,
                 own_send, own_recv, cols_send, cols_recv, w_send, w_recv):
    rows, columns = lax.axis_size("row"), lax.axis_size("col")
    r, c = lax.axis_index("row"), lax.axis_index("col")
    q, x = r // 2, r % 2
    other = r + 1 - 2 * x
    partner = c + 1 - 2 * (c % 2)
    odd = c % 2 == 1
    even = jnp.logical_not(odd)
    width = own_ref.shape[0]
    top = r == 0
    below = jnp.logical_not(top)
    corner = top & (c == 0)

    links = [
        ((r, partner), partner >= 0), ((other, c), other >= 0),
        ((r - 2, c), r >= 2), ((r + 2, c), r + 2 < rows),
        ((r, c - 2), c >= 2), ((r, c + 2), c + 2 < columns),
    ]
    barrier = pltpu.get_barrier_semaphore()
    for device, exists in links:
        @pl.when(exists)
        def _():
            pl.semaphore_signal(barrier, inc=1, device_id=device, device_id_type=MESH)
    peers = sum(jnp.where(exists, 1, 0).astype(jnp.int32) for _, exists in links)
    pl.semaphore_wait(barrier, peers)

    def send(source, target, send_sem, recv_sem, device):
        return pltpu.make_async_remote_copy(
            src_ref=source, dst_ref=target, send_sem=send_sem, recv_sem=recv_sem,
            device_id=device, device_id_type=MESH,
        )

    def start(condition, copies):
        for exists, copy in copies:
            @pl.when(condition & exists)
            def _():
                copy.start()

    side_row = jnp.where(x == 0, r + 1, r - 2)
    has_side = ((x == 0) & (q >= 1)) | (r == 3)

    steps = width // NB
    tall = NB // 2
    pieces = [
        (pl.ds(p * NB + h * tall, tall), pl.ds(j * NB, NB)) for p in range(steps) for j in range(p + 1) for h in range(2)
    ]

    def row_pieces(p):
        return range(p * (p + 1), (p + 1) * (p + 2))

    def w_first(m):
        part = w_ref.at[pieces[m]]
        return send(part, part, w_send.at[0], w_recv.at[m], (r, c + 1))

    def w_copies(m):
        part = w_ref.at[pieces[m]]

        def to(n, device):
            return send(part, part, w_send.at[n], w_recv.at[m], device)

        return [
            ((c == 1) & (x == 0) & (r + 2 < rows), to(0, (r + 2, c))),
            ((c == 1) & has_side, to(1, (side_row, c))),
            (c + 2 < columns, to(2, (r, c + 2))),
            (jnp.logical_not(top & (c == 1)), to(3, (r, c - 1))),
        ]

    def w_relay(m):
        copies = w_copies(m)
        copies[0][1].wait_recv()
        start(r >= 0, copies)

    deep = width // PANELS

    def own_part(j):
        return own_ref.at[pl.ds(pl.multiple_of(j * deep, deep), deep), :]

    def own_source(j):
        return mine_ref.at[pl.ds(pl.multiple_of(j * deep, deep), deep), pl.ds(0, width)]

    def own_load(j):
        return pltpu.make_async_copy(own_source(j), own_part(j), own_recv.at[j])

    def own_copies(j, source):
        def to(n, device):
            return send(source, own_part(j), own_send.at[n], own_recv.at[j], device)

        return [(c + 2 < columns, to(0, (r, c + 2))), (c >= 0, to(1, (r, c + 1)))]

    def own_wait(j):
        own_copies(j, own_part(j))[0][1].wait_recv()

    piece = width // CHUNKS

    def cols_part(ref, n, i):
        return ref.at[pl.ds(i * piece, piece), pl.ds(n * width, width)]

    def cols_copies(n, i, source):
        def to(m, device):
            return send(source, cols_part(cols_ref, n, i), cols_send.at[2 * n + m], cols_recv.at[n, i], device)

        return [((x == n) & (r + 2 < rows), to(0, (r + 2, c))), ((x == n) & (q >= 1) | (r == 3) & (n == 0), to(1, (sides[n], c)))]

    sides = [side_row, r - 1]
    relays = [(c > 0) & (((x == 0) & (q >= 1)) | (r == 3)), x == 1]

    def cols_first(n, i):
        source = cols_part(mine_ref, n, i)
        return send(source, cols_part(cols_ref, n, i), cols_send.at[2 * n], cols_recv.at[n, i], (r + 2 - n, c))

    def cols_wait(n, i):
        cols_first(n, i).wait_recv()

    def arrived(e):
        for n in range(2):
            @pl.when(jnp.logical_not(relays[n]) & ((c > 0) | (n == 1)))
            def _():
                for i in range((e - half) // piece, e // piece):
                    cols_wait(n, i)

    half = width // 2

    def log_det():
        here = lax.broadcasted_iota(jnp.int32, (NB, NB), 0) == lax.broadcasted_iota(jnp.int32, (NB, NB), 1)
        blocks = [slice(p * NB, (p + 1) * NB) for p in range(steps)]
        logs = sum(jnp.log(jnp.where(here, w_ref[at, at], 1.0)) for at in blocks)
        across = jnp.sum(logs, axis=0, keepdims=True)
        logdet_ref[...] = jnp.broadcast_to(-2.0 * jnp.sum(across, axis=1, keepdims=True), logdet_ref.shape)

    def panel(e, at=slice(None)):
        own = split(own_ref[at, :e])
        panel_ref[at, e - half : e] = dot_split(own, split(w_ref[e - half : e, :e]), 1)

    def block_row(e, at=slice(None)):
        other_ref[e - half : e, at] = dot_split(split(w_ref[e - half : e, :e]), split(cols_ref[:e, at]), 0)

    def update(at=slice(None)):
        rest_ref[:, at] = mine_ref[:, at] - dot_nn(panel_ref[:, :half], other_ref[:half, at])

    for p in range(steps):
        if p * NB % half == 0 and half > NB:
            w_ref[p * NB : (p + 1) * NB, (p + 1) * NB : p * NB + half] = jnp.zeros((NB, half - NB), jnp.float32)

    @pl.when(top)
    def _():
        for i in range(CHUNKS):
            cols_first(1, i).start()

            @pl.when(c > 0)
            def _():
                cols_first(0, i).start()

    @pl.when(below & (c == 0))
    def _():
        for j in range(PANELS):
            start(c >= 0, own_copies(j, own_source(j)))
        for j in range(PANELS):
            own_load(j).start()

    def w_leave(p):
        for m in row_pieces(p):
            w_first(m).start()

    @pl.when(corner)
    def _():
        factor_all(mine_ref, l_ref, w_ref, work, upper, inverse, w_leave)
        log_det()
        w_leave(steps - 1)

    @pl.when(top & odd)
    def _():
        for m in range(len(pieces)):
            w_relay(m)

    @pl.when(top & even & (c > 0))
    def _():
        for m in range(len(pieces)):
            w_first(m).wait_recv()

    first_half = row_pieces(half // NB)[0]
    patient = r == 1
    between = (x == 1) & (r + 2 >= rows)

    def w_arrive(first, last):
        @pl.when(even)
        def _():
            for m in range(first, last):
                w_first(m).wait_recv()

    def panel_arrive():
        @pl.when(c == 0)
        def _():
            for j in range(PANELS):
                own_load(j).wait()

        @pl.when(odd)
        def _():
            for j in range(PANELS):
                own_wait(j)

    lower = [slice(i, i + half) for i in range(0, 2 * width, half)]
    rows_of, right = lower[: width // half], lower[width // half :]
    items = [functools.partial(block_row, half, at) for at in right + rows_of]
    items += [functools.partial(panel, half, at) for at in rows_of]
    items += [functools.partial(update, at) for at in right + rows_of]

    @pl.when(below)
    def _():
        for i in range(CHUNKS):
            for n in range(2):
                @pl.when(relays[n])
                def _():
                    cols_wait(n, i)
                    start(c >= 0, cols_copies(n, i, cols_part(cols_ref, n, i)))

            for hop in range(1, HOPS + 1):
                j = i - min(FIRST + DELAY * (hop - 1), LAST)
                if 0 <= j < PANELS:
                    @pl.when(even & (c == 2 * hop if hop < HOPS else c >= 2 * hop))
                    def _():
                        own_wait(j)
                        start(c >= 0, own_copies(j, own_part(j)))

            for m, turn in enumerate(TURNS):
                for late, plane in ((0, c == 1), (WAIT, c > 1)):
                    if turn + late == i and (late == 0 or m < FOLLOW):
                        @pl.when(odd & plane & jnp.logical_not(patient))
                        def _():
                            w_relay(m)

            if i == MIDDLE:
                @pl.when(between)
                def _():
                    w_arrive(0, first_half)
                    panel_arrive()
                    arrived(half)

            if MIDDLE <= i < MIDDLE + len(items):
                pl.when(between)(items[i - MIDDLE])

        @pl.when(patient & odd)
        def _():
            for m in range(len(pieces)):
                w_relay(m)

        @pl.when(jnp.logical_not(between))
        def _():
            w_arrive(0, first_half)
            panel_arrive()
            arrived(half)
            block_row(half)
            panel(half)
            update()

        @pl.when(odd & (c > 1) & jnp.logical_not(patient))
        def _():
            for m in range(FOLLOW, len(pieces)):
                w_relay(m)

        w_arrive(first_half, len(pieces))
        panel(width)
        for n in range(2):
            @pl.when(x == n)
            def _():
                block_row(width, slice(n * width, (n + 1) * width))
                arrived(width)
                block_row(width, slice((1 - n) * width, (2 - n) * width))

    @pl.when(jnp.logical_not(corner))
    def _():
        log_det()

    def sent(condition, part, sem):
        @pl.when(condition)
        def _():
            send(part, part, sem, w_recv.at[0], (r, partner)).wait_send()

    inverse_part = cols_ref.at[pl.ds(0, (steps + 1) * NB // 4), :]
    sent(corner, inverse_part, w_send.at[0])
    for n, (exists, _) in enumerate(w_copies(0)):
        sent(odd & exists, inverse_part, w_send.at[n])
    for n, (exists, _) in enumerate(own_copies(0, own_part(0))):
        sent(below & even & exists, own_ref, own_send.at[n])
    for n in range(2):
        part = cols_ref.at[:, pl.ds(n * width, width)]
        sent(top & ((c > 0) | (n == 1)), part, cols_send.at[2 * n])
        for m, (exists, _) in enumerate(cols_copies(n, 0, cols_part(cols_ref, n, 0))):
            sent(below & relays[n] & exists, part, cols_send.at[2 * n + m])


def panel_step(mine):
    width = mine.shape[0]
    square = jax.ShapeDtypeStruct((width, width), jnp.float32)
    wide = (width, 2 * width)
    dma = pltpu.SemaphoreType.DMA
    pieces = (width // NB) * (width // NB + 1)
    return pl.pallas_call(
        panel_kernel,
        out_shape=(
            square, jax.ShapeDtypeStruct(wide, jnp.float32), jax.ShapeDtypeStruct(wide, jnp.float32), square,
            jax.ShapeDtypeStruct((1, NB), jnp.float32),
        ),
        in_specs=[VMEM],
        out_specs=(VMEM,) * 5,
        scratch_shapes=[
            pltpu.VMEM((width, width), jnp.float32), pltpu.VMEM(wide, jnp.float32),
            pltpu.VMEM((width, width), jnp.float32), pltpu.VMEM((width, width), jnp.float32),
            pltpu.VMEM((NB, NB), jnp.float32), pltpu.VMEM((NB, NB), jnp.float32),
            dma((2,)), dma((PANELS,)), dma((4,)), dma((2, CHUNKS)), dma((4,)), dma((pieces,)),
        ],
        compiler_params=pltpu.CompilerParams(collective_id=0, has_side_effects=True, vmem_limit_bytes=30 << 20),
    )(mine)


def per_device(mine):
    panel, other, rest, l, logdet = panel_step(mine)
    width = mine.shape[0]
    across = pl.BlockSpec((width, width), lambda s: (0, s))
    whole = pl.BlockSpec((width, width), lambda s: (0, 0))
    block = pl.pallas_call(
        update_kernel,
        grid=(mine.shape[1] // width,),
        out_shape=jax.ShapeDtypeStruct(mine.shape, jnp.float32),
        in_specs=[across, whole, across, whole],
        out_specs=across,
        compiler_params=pltpu.CompilerParams(vmem_limit_bytes=16 << 20),
    )(rest, panel, other, l)
    return block, logdet[0, 0]


def solution(mesh):
    return jax.shard_map(
        per_device, mesh=mesh, in_specs=(P("row", "col"),), out_specs=(P("row", "col"), P()), check_vma=False
    )
```

```python
import functools

import jax
import jax.numpy as jnp
from jax import lax
from jax.experimental import pallas as pl
from jax.experimental.pallas import tpu as pltpu
from jax.sharding import PartitionSpec as P

MESH = pl.DeviceIdType.MESH
NB = 128
BAND = 32
CHUNKS = 32
PANELS = 16
HOPS = 2
FIRST = 2
DELAY = 3
LAST = 5
TURNS = (10, 11, 15, 16, 17, 18, 21, 21, 22, 22, 23, 24, 24, 25, 25, 26, 26, 27, 27, 28)
FOLLOW = 12
WAIT = 3
MIDDLE = 22
VMEM = pl.BlockSpec(memory_space=pltpu.VMEM)


def split(a):
    high = a.astype(jnp.bfloat16)
    return high, (a - high.astype(jnp.float32)).astype(jnp.bfloat16)


def dot_split(a, b, axis):
    def dot(u, v):
        return lax.dot_general(u, v, (((1,), (axis,)), ((), ())), preferred_element_type=jnp.float32)

    return dot(a[0], b[0]) + (dot(a[0], b[1]) + dot(a[1], b[0]))


def dot_nt(a, b):
    return dot_split(split(a), split(b), 1)


def dot_nn(a, b):
    return dot_split(split(a), split(b), 0)


def total(terms):
    while len(terms) > 1:
        terms = [a + b for a, b in zip(terms[::2], terms[1::2])]
    return terms[0]


def eliminate(left, right, base):
    sub = lax.broadcasted_iota(jnp.int32, (8, NB), 0)
    left, right = list(left), list(right)
    upper, inverse = [], []

    def row(x, t):
        return jnp.take_along_axis(x, jnp.full((8, NB), t, jnp.int32), axis=0)

    def column(x, t):
        return jnp.broadcast_to(x[:, t : t + 1], (8, NB))

    for p in range(0, len(left), 2):
        first = base + 8 * p
        rest = range(p + 2, len(left))
        cols = [[column(x, first + t) for x in left[p : p + 2]] for t in range(16)]
        mult = {g: [column(left[g], first + t) for t in range(16)] for g in rest}
        v, i = left[p : p + 2], right[p : p + 2]
        u_rows, i_rows, d_rows = list(v), list(i), [None, None]
        for t in range(16):
            at, s = t // 8, t % 8
            here = sub == s
            pivot = row(cols[t][at], s)
            if s:
                u_rows[at] = jnp.where(here, v[at], u_rows[at])
                i_rows[at] = jnp.where(here, i[at], i_rows[at])
                d_rows[at] = jnp.where(here, pivot, d_rows[at])
            else:
                u_rows[at], i_rows[at], d_rows[at] = v[at], i[at], pivot
            recip = 1.0 / pivot
            factor = [x * recip for x in cols[t]]
            factor[at] = jnp.where(here, -recip, factor[at])

            def step(pair):
                taken = row(pair[at], s)
                kept = [jnp.where(here, 0.0, x) if h == at else x for h, x in enumerate(pair)]
                return [x - f * taken for x, f in zip(kept, factor)]

            for w in range(t + 1, 16):
                cols[w] = step(cols[w])
            v, i = step(v), step(i)
        for h in range(2):
            scale = lax.rsqrt(d_rows[h])
            upper.append(u_rows[h] * scale)
            inverse.append(i_rows[h] * scale)
        v_rows = [row(v[t // 8], t % 8) for t in range(16)]
        i_rows = [row(i[t // 8], t % 8) for t in range(16)]
        for g in rest:
            left[g] = left[g] - total([mult[g][t] * v_rows[t] for t in range(16)])
            right[g] = right[g] - total([mult[g][t] * i_rows[t] for t in range(16)])
    return upper, inverse


def factor_block(a):
    lane = lax.broadcasted_iota(jnp.int32, (NB, NB), 1)
    sub = lax.broadcasted_iota(jnp.int32, (NB, NB), 0)
    left, right = a, (lane == sub).astype(jnp.float32)
    upper, inverse = [], []
    for base in range(0, NB, BAND):
        rows = [slice(8 * g, 8 * g + 8) for g in range(BAND // 8)]
        u, i = eliminate([left[x] for x in rows], [right[x] for x in rows], base)
        u, i = jnp.concatenate(u, 0), jnp.concatenate(i, 0)
        upper.append(u)
        inverse.append(i)
        if base + BAND < NB:
            change = dot_nn(u.T[base + BAND :, :], jnp.concatenate([u, i], 1))
            left, right = left[BAND:] - change[:, :NB], right[BAND:] - change[:, NB:]
    upper = jnp.where(lane >= sub, jnp.concatenate(upper, 0), 0.0)
    return upper, jnp.concatenate(inverse, 0)


def factor_all(a_ref, l_ref, w_ref, work, upper, inverse, leave):
    size = w_ref.shape[0]
    work[:NB, :NB] = a_ref[:NB, :NB]
    l_ref[...] = jnp.zeros_like(l_ref)

    @pl.loop(0, size // NB)
    def _(step):
        span = pl.ds(pl.multiple_of(step * NB, NB), NB)
        r, w = factor_block(work[span, span])
        upper[...] = r
        inverse[...] = w
        w_ref[span, span] = inverse[...]
        l_ref[span, span] = upper[...].T
        for p in range(size // NB):

            @pl.when(step == p)
            def _():
                at = slice(p * NB, (p + 1) * NB)
                end = (p + 1) * NB
                if p:
                    leave(p - 1)
                if end < size:
                    below = work[end:, at] if p else a_ref[end:, at]
                    l_ref[end:, at] = dot_nt(below, inverse[...])
                    following = slice(end, end + NB)
                    work[end:, following] = a_ref[end:, following] - dot_nt(l_ref[end:, :end], l_ref[following, :end])
                if p:
                    inner = dot_nn(l_ref[at, : p * NB], w_ref[: p * NB, : p * NB])
                    w_ref[at, : p * NB] = -dot_nn(inverse[...], inner)


def panel_kernel(mine_ref, rest_ref, logdet_ref,
                 panel_ref, other_ref, l_ref, own_ref, cols_ref, w_ref, work, upper, inverse,
                 own_send, own_recv, cols_send, cols_recv, w_send, w_recv, load_sem):
    rows, columns = lax.axis_size("row"), lax.axis_size("col")
    r, c = lax.axis_index("row"), lax.axis_index("col")
    q, x = r // 2, r % 2
    other = r + 1 - 2 * x
    partner = c + 1 - 2 * (c % 2)
    odd = c % 2 == 1
    even = jnp.logical_not(odd)
    width = own_ref.shape[0]
    top = r == 0
    below = jnp.logical_not(top)
    corner = top & (c == 0)

    links = [
        ((r, partner), partner >= 0), ((other, c), other >= 0),
        ((r - 2, c), r >= 2), ((r + 2, c), r + 2 < rows),
        ((r, c - 2), c >= 2), ((r, c + 2), c + 2 < columns),
    ]
    barrier = pltpu.get_barrier_semaphore()
    for device, exists in links:
        @pl.when(exists)
        def _():
            pl.semaphore_signal(barrier, inc=1, device_id=device, device_id_type=MESH)
    peers = sum(jnp.where(exists, 1, 0).astype(jnp.int32) for _, exists in links)
    pl.semaphore_wait(barrier, peers)

    def send(source, target, send_sem, recv_sem, device):
        return pltpu.make_async_remote_copy(
            src_ref=source, dst_ref=target, send_sem=send_sem, recv_sem=recv_sem,
            device_id=device, device_id_type=MESH,
        )

    def start(condition, copies):
        for exists, copy in copies:
            @pl.when(condition & exists)
            def _():
                copy.start()

    side_row = jnp.where(x == 0, r + 1, r - 2)
    has_side = ((x == 0) & (q >= 1)) | (r == 3)

    steps = width // NB
    tall = NB // 2
    pieces = [
        (pl.ds(p * NB + h * tall, tall), pl.ds(j * NB, NB)) for p in range(steps) for j in range(p + 1) for h in range(2)
    ]

    def row_pieces(p):
        return range(p * (p + 1), (p + 1) * (p + 2))

    def w_first(m):
        part = w_ref.at[pieces[m]]
        return send(part, part, w_send.at[0], w_recv.at[m], (r, c + 1))

    def w_copies(m):
        part = w_ref.at[pieces[m]]

        def to(n, device):
            return send(part, part, w_send.at[n], w_recv.at[m], device)

        return [
            ((c == 1) & (x == 0) & (r + 2 < rows), to(0, (r + 2, c))),
            ((c == 1) & has_side, to(1, (side_row, c))),
            (c + 2 < columns, to(2, (r, c + 2))),
            (jnp.logical_not(top & (c == 1)), to(3, (r, c - 1))),
        ]

    def w_relay(m):
        copies = w_copies(m)
        copies[0][1].wait_recv()
        start(r >= 0, copies)

    deep = width // PANELS

    def own_part(j):
        return own_ref.at[pl.ds(pl.multiple_of(j * deep, deep), deep), :]

    def own_source(j):
        return mine_ref.at[pl.ds(pl.multiple_of(j * deep, deep), deep), pl.ds(0, width)]

    def own_load(j):
        return pltpu.make_async_copy(own_source(j), own_part(j), own_recv.at[j])

    def own_copies(j, source):
        def to(n, device):
            return send(source, own_part(j), own_send.at[n], own_recv.at[j], device)

        return [(c + 2 < columns, to(0, (r, c + 2))), (c >= 0, to(1, (r, c + 1)))]

    def own_wait(j):
        own_copies(j, own_part(j))[0][1].wait_recv()

    piece = width // CHUNKS

    def cols_part(ref, n, i):
        return ref.at[pl.ds(i * piece, piece), pl.ds(n * width, width)]

    def cols_copies(n, i, source):
        def to(m, device):
            return send(source, cols_part(cols_ref, n, i), cols_send.at[2 * n + m], cols_recv.at[n, i], device)

        return [((x == n) & (r + 2 < rows), to(0, (r + 2, c))), ((x == n) & (q >= 1) | (r == 3) & (n == 0), to(1, (sides[n], c)))]

    sides = [side_row, r - 1]
    relays = [(c > 0) & (((x == 0) & (q >= 1)) | (r == 3)), x == 1]

    def cols_first(n, i):
        source = cols_part(mine_ref, n, i)
        return send(source, cols_part(cols_ref, n, i), cols_send.at[2 * n], cols_recv.at[n, i], (r + 2 - n, c))

    def cols_wait(n, i):
        cols_first(n, i).wait_recv()

    def arrived(e):
        for n in range(2):
            @pl.when(jnp.logical_not(relays[n]) & ((c > 0) | (n == 1)))
            def _():
                for i in range((e - half) // piece, e // piece):
                    cols_wait(n, i)

    half = width // 2

    def log_det():
        here = lax.broadcasted_iota(jnp.int32, (NB, NB), 0) == lax.broadcasted_iota(jnp.int32, (NB, NB), 1)
        blocks = [slice(p * NB, (p + 1) * NB) for p in range(steps)]
        logs = sum(jnp.log(jnp.where(here, w_ref[at, at], 1.0)) for at in blocks)
        across = jnp.sum(logs, axis=0, keepdims=True)
        logdet_ref[...] = jnp.broadcast_to(-2.0 * jnp.sum(across, axis=1, keepdims=True), logdet_ref.shape)

    def panel(e, at=slice(None)):
        own = split(own_ref[at, :e])
        panel_ref[at, e - half : e] = dot_split(own, split(w_ref[e - half : e, :e]), 1)

    def block_row(e, at=slice(None)):
        other_ref[e - half : e, at] = dot_split(split(w_ref[e - half : e, :e]), split(cols_ref[:e, at]), 0)

    mine_load = pltpu.make_async_copy(mine_ref, rest_ref, load_sem)

    def update(at=slice(None)):
        rest_ref[:, at] = rest_ref[:, at] - dot_nn(panel_ref[:, :half], other_ref[:half, at])

    def finish(at):
        block_row(width, at)
        rest_ref[:, at] = rest_ref[:, at] - dot_nn(panel_ref[:, half:], other_ref[half:, at])

    for p in range(steps):
        if p * NB % half == 0 and half > NB:
            w_ref[p * NB : (p + 1) * NB, (p + 1) * NB : p * NB + half] = jnp.zeros((NB, half - NB), jnp.float32)

    diagonal_load = pltpu.make_async_copy(mine_ref.at[:, pl.ds(0, width)], own_ref, load_sem)

    @pl.when(corner)
    def _():
        diagonal_load.start()

    @pl.when(top)
    def _():
        for i in range(CHUNKS):
            cols_first(1, i).start()

            @pl.when(c > 0)
            def _():
                cols_first(0, i).start()

    @pl.when(below & (c == 0))
    def _():
        for j in range(PANELS):
            start(c >= 0, own_copies(j, own_source(j)))
        for j in range(PANELS):
            own_load(j).start()

    @pl.when(below)
    def _():
        mine_load.start()

    def w_leave(p):
        for m in row_pieces(p):
            w_first(m).start()

    @pl.when(corner)
    def _():
        diagonal_load.wait()
        factor_all(own_ref, l_ref, w_ref, work, upper, inverse, w_leave)
        log_det()
        w_leave(steps - 1)

    @pl.when(top & odd)
    def _():
        for m in range(len(pieces)):
            w_relay(m)

    @pl.when(top & even & (c > 0))
    def _():
        for m in range(len(pieces)):
            w_first(m).wait_recv()

    first_half = row_pieces(half // NB)[0]
    patient = r == 1
    between = (x == 1) & (r + 2 >= rows)

    def w_arrive(first, last):
        @pl.when(even)
        def _():
            for m in range(first, last):
                w_first(m).wait_recv()

    def panel_arrive():
        mine_load.wait()

        @pl.when(c == 0)
        def _():
            for j in range(PANELS):
                own_load(j).wait()

        @pl.when(odd)
        def _():
            for j in range(PANELS):
                own_wait(j)

    lower = [slice(i, i + half) for i in range(0, 2 * width, half)]
    rows_of, right = lower[: width // half], lower[width // half :]
    items = [functools.partial(block_row, half, at) for at in right + rows_of]
    items += [functools.partial(panel, half, at) for at in rows_of]
    items += [functools.partial(update, at) for at in right + rows_of]

    @pl.when(below)
    def _():
        for i in range(CHUNKS):
            for n in range(2):
                @pl.when(relays[n])
                def _():
                    cols_wait(n, i)
                    start(c >= 0, cols_copies(n, i, cols_part(cols_ref, n, i)))

            for hop in range(1, HOPS + 1):
                j = i - min(FIRST + DELAY * (hop - 1), LAST)
                if 0 <= j < PANELS:
                    @pl.when(even & (c == 2 * hop if hop < HOPS else c >= 2 * hop))
                    def _():
                        own_wait(j)
                        start(c >= 0, own_copies(j, own_part(j)))

            for m, turn in enumerate(TURNS):
                for late, plane in ((0, c == 1), (WAIT, c > 1)):
                    if turn + late == i and (late == 0 or m < FOLLOW):
                        @pl.when(odd & plane & jnp.logical_not(patient))
                        def _():
                            w_relay(m)

            if i == MIDDLE:
                @pl.when(between)
                def _():
                    w_arrive(0, first_half)
                    panel_arrive()
                    arrived(half)

            if MIDDLE <= i < MIDDLE + len(items):
                pl.when(between)(items[i - MIDDLE])

        @pl.when(patient & odd)
        def _():
            for m in range(len(pieces)):
                w_relay(m)

        @pl.when(jnp.logical_not(between))
        def _():
            w_arrive(0, first_half)
            panel_arrive()
            arrived(half)
            block_row(half)
            panel(half)
            update()

        @pl.when(odd & (c > 1) & jnp.logical_not(patient))
        def _():
            for m in range(FOLLOW, len(pieces)):
                w_relay(m)

        w_arrive(first_half, len(pieces))
        panel(width)
        for n in range(2):
            @pl.when(x == n)
            def _():
                finish(slice(n * width, (n + 1) * width))
                arrived(width)
                finish(slice((1 - n) * width, (2 - n) * width))

        @pl.when(c == 0)
        def _():
            rest_ref[:, :width] = panel_ref[...]

    @pl.when(top)
    def _():
        rest_ref[...] = jnp.zeros_like(rest_ref)

    @pl.when(corner)
    def _():
        rest_ref[:, :width] = l_ref[...]

    @pl.when(jnp.logical_not(corner))
    def _():
        log_det()

    def sent(condition, part, sem):
        @pl.when(condition)
        def _():
            send(part, part, sem, w_recv.at[0], (r, partner)).wait_send()

    inverse_part = cols_ref.at[pl.ds(0, (steps + 1) * NB // 4), :]
    sent(corner, inverse_part, w_send.at[0])
    for n, (exists, _) in enumerate(w_copies(0)):
        sent(odd & exists, inverse_part, w_send.at[n])
    for n, (exists, _) in enumerate(own_copies(0, own_part(0))):
        sent(below & even & exists, own_ref, own_send.at[n])
    for n in range(2):
        part = cols_ref.at[:, pl.ds(n * width, width)]
        sent(top & ((c > 0) | (n == 1)), part, cols_send.at[2 * n])
        for m, (exists, _) in enumerate(cols_copies(n, 0, cols_part(cols_ref, n, 0))):
            sent(below & relays[n] & exists, part, cols_send.at[2 * n + m])


def panel_step(mine):
    width = mine.shape[0]
    square = jax.ShapeDtypeStruct((width, width), jnp.float32)
    wide = (width, 2 * width)
    dma = pltpu.SemaphoreType.DMA
    pieces = (width // NB) * (width // NB + 1)
    return pl.pallas_call(
        panel_kernel,
        out_shape=(jax.ShapeDtypeStruct(wide, jnp.float32), jax.ShapeDtypeStruct((1, NB), jnp.float32)),
        in_specs=[pl.BlockSpec(memory_space=pltpu.HBM)],
        out_specs=(VMEM,) * 2,
        scratch_shapes=[
            pltpu.VMEM((width, width), jnp.float32), pltpu.VMEM(wide, jnp.float32), pltpu.VMEM((width, width), jnp.float32),
            pltpu.VMEM((width, width), jnp.float32), pltpu.VMEM(wide, jnp.float32),
            pltpu.VMEM((width, width), jnp.float32), pltpu.VMEM((width, width), jnp.float32),
            pltpu.VMEM((NB, NB), jnp.float32), pltpu.VMEM((NB, NB), jnp.float32),
            dma((2,)), dma((PANELS,)), dma((4,)), dma((2, CHUNKS)), dma((4,)), dma((pieces,)), dma(()),
        ],
        compiler_params=pltpu.CompilerParams(collective_id=0, has_side_effects=True, vmem_limit_bytes=50 << 20),
    )(mine)


def per_device(mine):
    block, logdet = panel_step(mine)
    return block, logdet[0, 0]


def solution(mesh):
    return jax.shard_map(
        per_device, mesh=mesh, in_specs=(P("row", "col"),), out_specs=(P("row", "col"), P()), check_vma=False
    )
```

```python
import functools

import jax
import jax.numpy as jnp
from jax import lax
from jax.experimental import pallas as pl
from jax.experimental.pallas import tpu as pltpu
from jax.sharding import PartitionSpec as P

MESH = pl.DeviceIdType.MESH
NB = 128
BAND = 32
CHUNKS = 32
PANELS = 16
HOPS = 2
FIRST = 2
DELAY = 3
LAST = 5
TURNS = (10, 11, 15, 16, 17, 18, 21, 21, 22, 22, 23, 24, 24, 25, 25, 26, 26, 27, 27, 28)
FOLLOW = 12
WAIT = 3
MIDDLE = 22
VMEM = pl.BlockSpec(memory_space=pltpu.VMEM)


def split(a):
    high = a.astype(jnp.bfloat16)
    return high, (a - high.astype(jnp.float32)).astype(jnp.bfloat16)


def dot_split(a, b, axis):
    def dot(u, v):
        return lax.dot_general(u, v, (((1,), (axis,)), ((), ())), preferred_element_type=jnp.float32)

    return dot(a[0], b[0]) + (dot(a[0], b[1]) + dot(a[1], b[0]))


def dot_nt(a, b):
    return dot_split(split(a), split(b), 1)


def dot_nn(a, b):
    return dot_split(split(a), split(b), 0)


def total(terms):
    while len(terms) > 1:
        terms = [a + b for a, b in zip(terms[::2], terms[1::2])]
    return terms[0]


def eliminate(left, right, base):
    sub = lax.broadcasted_iota(jnp.int32, (8, NB), 0)
    left, right = list(left), list(right)
    upper, inverse = [], []

    def row(x, t):
        return jnp.take_along_axis(x, jnp.full((8, NB), t, jnp.int32), axis=0)

    def column(x, t):
        return jnp.broadcast_to(x[:, t : t + 1], (8, NB))

    for p in range(0, len(left), 2):
        first = base + 8 * p
        rest = range(p + 2, len(left))
        cols = [[column(x, first + t) for x in left[p : p + 2]] for t in range(16)]
        mult = {g: [column(left[g], first + t) for t in range(16)] for g in rest}
        v, i = left[p : p + 2], right[p : p + 2]
        u_rows, i_rows, d_rows = list(v), list(i), [None, None]
        for t in range(16):
            at, s = t // 8, t % 8
            here = sub == s
            pivot = row(cols[t][at], s)
            if s:
                u_rows[at] = jnp.where(here, v[at], u_rows[at])
                i_rows[at] = jnp.where(here, i[at], i_rows[at])
                d_rows[at] = jnp.where(here, pivot, d_rows[at])
            else:
                u_rows[at], i_rows[at], d_rows[at] = v[at], i[at], pivot
            recip = 1.0 / pivot
            factor = [x * recip for x in cols[t]]
            factor[at] = jnp.where(here, -recip, factor[at])

            def step(pair):
                taken = row(pair[at], s)
                kept = [jnp.where(here, 0.0, x) if h == at else x for h, x in enumerate(pair)]
                return [x - f * taken for x, f in zip(kept, factor)]

            for w in range(t + 1, 16):
                cols[w] = step(cols[w])
            v, i = step(v), step(i)
        for h in range(2):
            scale = lax.rsqrt(d_rows[h])
            upper.append(u_rows[h] * scale)
            inverse.append(i_rows[h] * scale)
        v_rows = [row(v[t // 8], t % 8) for t in range(16)]
        i_rows = [row(i[t // 8], t % 8) for t in range(16)]
        for g in rest:
            left[g] = left[g] - total([mult[g][t] * v_rows[t] for t in range(16)])
            right[g] = right[g] - total([mult[g][t] * i_rows[t] for t in range(16)])
    return upper, inverse


def factor_block(a):
    lane = lax.broadcasted_iota(jnp.int32, (NB, NB), 1)
    sub = lax.broadcasted_iota(jnp.int32, (NB, NB), 0)
    left, right = a, (lane == sub).astype(jnp.float32)
    upper, inverse = [], []
    for base in range(0, NB, BAND):
        rows = [slice(8 * g, 8 * g + 8) for g in range(BAND // 8)]
        u, i = eliminate([left[x] for x in rows], [right[x] for x in rows], base)
        u, i = jnp.concatenate(u, 0), jnp.concatenate(i, 0)
        upper.append(u)
        inverse.append(i)
        if base + BAND < NB:
            change = dot_nn(u.T[base + BAND :, :], jnp.concatenate([u, i], 1))
            left, right = left[BAND:] - change[:, :NB], right[BAND:] - change[:, NB:]
    upper = jnp.where(lane >= sub, jnp.concatenate(upper, 0), 0.0)
    return upper, jnp.concatenate(inverse, 0)


def factor_all(a_ref, l_ref, w_ref, work, upper, inverse, leave):
    size = w_ref.shape[0]
    work[:NB, :NB] = a_ref[:NB, :NB]
    l_ref[...] = jnp.zeros_like(l_ref)

    @pl.loop(0, size // NB)
    def _(step):
        span = pl.ds(pl.multiple_of(step * NB, NB), NB)
        r, w = factor_block(work[span, span])
        upper[...] = r
        inverse[...] = w
        w_ref[span, span] = inverse[...]
        l_ref[span, span] = upper[...].T
        for p in range(size // NB):

            @pl.when(step == p)
            def _():
                at = slice(p * NB, (p + 1) * NB)
                end = (p + 1) * NB
                if p:
                    leave(p - 1)
                if end < size:
                    below = work[end:, at] if p else a_ref[end:, at]
                    l_ref[end:, at] = dot_nt(below, inverse[...])
                    following = slice(end, end + NB)
                    work[end:, following] = a_ref[end:, following] - dot_nt(l_ref[end:, :end], l_ref[following, :end])
                if p:
                    inner = dot_nn(l_ref[at, : p * NB], w_ref[: p * NB, : p * NB])
                    w_ref[at, : p * NB] = -dot_nn(inverse[...], inner)


def panel_kernel(mine_ref, rest_ref, logdet_ref,
                 panel_ref, other_ref, l_ref, own_ref, cols_ref, w_ref, work, upper, inverse,
                 own_send, own_recv, cols_send, cols_recv, w_send, w_recv, load_sem):
    rows, columns = lax.axis_size("row"), lax.axis_size("col")
    r, c = lax.axis_index("row"), lax.axis_index("col")
    q, x = r // 2, r % 2
    other = r + 1 - 2 * x
    partner = c + 1 - 2 * (c % 2)
    odd = c % 2 == 1
    even = jnp.logical_not(odd)
    width = own_ref.shape[0]
    top = r == 0
    below = jnp.logical_not(top)
    corner = top & (c == 0)

    links = [
        ((r, partner), partner >= 0), ((other, c), other >= 0),
        ((r - 2, c), r >= 2), ((r + 2, c), r + 2 < rows),
        ((r, c - 2), c >= 2), ((r, c + 2), c + 2 < columns),
    ]
    barrier = pltpu.get_barrier_semaphore()
    for device, exists in links:
        @pl.when(exists)
        def _():
            pl.semaphore_signal(barrier, inc=1, device_id=device, device_id_type=MESH)
    peers = sum(jnp.where(exists, 1, 0).astype(jnp.int32) for _, exists in links)
    pl.semaphore_wait(barrier, peers)

    def send(source, target, send_sem, recv_sem, device):
        return pltpu.make_async_remote_copy(
            src_ref=source, dst_ref=target, send_sem=send_sem, recv_sem=recv_sem,
            device_id=device, device_id_type=MESH,
        )

    def start(condition, copies):
        for exists, copy in copies:
            @pl.when(condition & exists)
            def _():
                copy.start()

    side_row = jnp.where(x == 0, r + 1, r - 2)
    has_side = ((x == 0) & (q >= 1)) | (r == 3)

    steps = width // NB
    tall = NB // 2
    pieces = [
        (pl.ds(p * NB + h * tall, tall), pl.ds(j * NB, NB)) for p in range(steps) for j in range(p + 1) for h in range(2)
    ]

    def row_pieces(p):
        return range(p * (p + 1), (p + 1) * (p + 2))

    def w_first(m):
        part = w_ref.at[pieces[m]]
        return send(part, part, w_send.at[0], w_recv.at[m], (r, c + 1))

    def w_copies(m):
        part = w_ref.at[pieces[m]]

        def to(n, device):
            return send(part, part, w_send.at[n], w_recv.at[m], device)

        return [
            ((c == 1) & (x == 0) & (r + 2 < rows), to(0, (r + 2, c))),
            ((c == 1) & has_side, to(1, (side_row, c))),
            (c + 2 < columns, to(2, (r, c + 2))),
            (jnp.logical_not(top & (c == 1)), to(3, (r, c - 1))),
        ]

    def w_relay(m):
        copies = w_copies(m)
        copies[0][1].wait_recv()
        start(r >= 0, copies)

    deep = width // PANELS

    def own_part(j):
        return own_ref.at[pl.ds(pl.multiple_of(j * deep, deep), deep), :]

    def own_source(j):
        return mine_ref.at[pl.ds(pl.multiple_of(j * deep, deep), deep), pl.ds(0, width)]

    def own_load(j):
        return pltpu.make_async_copy(own_source(j), own_part(j), own_recv.at[j])

    def own_copies(j, source):
        def to(n, device):
            return send(source, own_part(j), own_send.at[n], own_recv.at[j], device)

        return [(c + 2 < columns, to(0, (r, c + 2))), (c >= 0, to(1, (r, c + 1)))]

    def own_wait(j):
        own_copies(j, own_part(j))[0][1].wait_recv()

    piece = width // CHUNKS

    def cols_part(ref, n, i):
        return ref.at[pl.ds(i * piece, piece), pl.ds(n * width, width)]

    def cols_copies(n, i, source):
        def to(m, device):
            return send(source, cols_part(cols_ref, n, i), cols_send.at[2 * n + m], cols_recv.at[n, i], device)

        return [((x == n) & (r + 2 < rows), to(0, (r + 2, c))), ((x == n) & (q >= 1) | (r == 3) & (n == 0), to(1, (sides[n], c)))]

    sides = [side_row, r - 1]
    relays = [(c > 0) & (((x == 0) & (q >= 1)) | (r == 3)), x == 1]

    def cols_first(n, i):
        source = cols_part(mine_ref, n, i)
        return send(source, cols_part(cols_ref, n, i), cols_send.at[2 * n], cols_recv.at[n, i], (r + 2 - n, c))

    def cols_wait(n, i):
        cols_first(n, i).wait_recv()

    def arrived(first, last):
        for n in range(2):
            @pl.when(jnp.logical_not(relays[n]) & ((c > 0) | (n == 1)))
            def _():
                for i in range(first // piece, last // piece):
                    cols_wait(n, i)

    half = width // 2

    def log_det():
        here = lax.broadcasted_iota(jnp.int32, (NB, NB), 0) == lax.broadcasted_iota(jnp.int32, (NB, NB), 1)
        blocks = [slice(p * NB, (p + 1) * NB) for p in range(steps)]
        logs = sum(jnp.log(jnp.where(here, w_ref[at, at], 1.0)) for at in blocks)
        across = jnp.sum(logs, axis=0, keepdims=True)
        logdet_ref[...] = jnp.broadcast_to(-2.0 * jnp.sum(across, axis=1, keepdims=True), logdet_ref.shape)

    def panel(e, at=slice(None)):
        own = split(own_ref[at, :e])
        panel_ref[at, e - half : e] = dot_split(own, split(w_ref[e - half : e, :e]), 1)

    def block_row(e, at=slice(None)):
        other_ref[e - half : e, at] = dot_split(split(w_ref[e - half : e, :e]), split(cols_ref[:e, at]), 0)

    mine_load = pltpu.make_async_copy(mine_ref, rest_ref, load_sem)

    def update(at=slice(None)):
        rest_ref[:, at] = rest_ref[:, at] - dot_nn(panel_ref[:, :half], other_ref[:half, at])

    def finish(at):
        block_row(width, at)
        rest_ref[:, at] = rest_ref[:, at] - dot_nn(panel_ref[:, half:], other_ref[half:, at])

    def finish_late(at):
        last = width - NB
        arrived(half, last)
        other_ref[half:, at] = dot_nn(w_ref[half:, :last], cols_ref[:last, at])
        rest_ref[:, at] = rest_ref[:, at] - dot_nn(panel_ref[:, half:last], other_ref[half:last, at])
        arrived(last, width)
        other_ref[last:, at] = other_ref[last:, at] + dot_nn(w_ref[last:, last:], cols_ref[last:, at])
        rest_ref[:, at] = rest_ref[:, at] - dot_nn(panel_ref[:, last:], other_ref[last:, at])

    for p in range(steps):
        if p * NB % half == 0 and half > NB:
            w_ref[p * NB : (p + 1) * NB, (p + 1) * NB : p * NB + half] = jnp.zeros((NB, half - NB), jnp.float32)

    diagonal_load = pltpu.make_async_copy(mine_ref.at[:, pl.ds(0, width)], own_ref, load_sem)

    @pl.when(corner)
    def _():
        diagonal_load.start()

    @pl.when(top)
    def _():
        for i in range(CHUNKS):
            cols_first(1, i).start()

            @pl.when(c > 0)
            def _():
                cols_first(0, i).start()

    @pl.when(below & (c == 0))
    def _():
        for j in range(PANELS):
            start(c >= 0, own_copies(j, own_source(j)))
        for j in range(PANELS):
            own_load(j).start()

    @pl.when(below)
    def _():
        mine_load.start()

    def w_leave(p):
        for m in row_pieces(p):
            w_first(m).start()

    @pl.when(corner)
    def _():
        diagonal_load.wait()
        factor_all(own_ref, l_ref, w_ref, work, upper, inverse, w_leave)
        log_det()
        w_leave(steps - 1)

    @pl.when(top & odd)
    def _():
        for m in range(len(pieces)):
            w_relay(m)

    @pl.when(top & even & (c > 0))
    def _():
        for m in range(len(pieces)):
            w_first(m).wait_recv()

    first_half = row_pieces(half // NB)[0]
    patient = r == 1
    between = (x == 1) & (r + 2 >= rows)

    def w_arrive(first, last):
        @pl.when(even)
        def _():
            for m in range(first, last):
                w_first(m).wait_recv()

    def panel_arrive():
        mine_load.wait()

        @pl.when(c == 0)
        def _():
            for j in range(PANELS):
                own_load(j).wait()

        @pl.when(odd)
        def _():
            for j in range(PANELS):
                own_wait(j)

    lower = [slice(i, i + half) for i in range(0, 2 * width, half)]
    rows_of, right = lower[: width // half], lower[width // half :]
    items = [functools.partial(block_row, half, at) for at in right + rows_of]
    items += [functools.partial(panel, half, at) for at in rows_of]
    items += [functools.partial(update, at) for at in right + rows_of]

    @pl.when(below)
    def _():
        for i in range(CHUNKS):
            for n in range(2):
                @pl.when(relays[n])
                def _():
                    cols_wait(n, i)
                    start(c >= 0, cols_copies(n, i, cols_part(cols_ref, n, i)))

            for hop in range(1, HOPS + 1):
                j = i - min(FIRST + DELAY * (hop - 1), LAST)
                if 0 <= j < PANELS:
                    @pl.when(even & (c == 2 * hop if hop < HOPS else c >= 2 * hop))
                    def _():
                        own_wait(j)
                        start(c >= 0, own_copies(j, own_part(j)))

            for m, turn in enumerate(TURNS):
                for late, plane in ((0, c == 1), (WAIT, c > 1)):
                    if turn + late == i and (late == 0 or m < FOLLOW):
                        @pl.when(odd & plane & jnp.logical_not(patient))
                        def _():
                            w_relay(m)

            if i == MIDDLE:
                @pl.when(between)
                def _():
                    w_arrive(0, first_half)
                    panel_arrive()
                    arrived(0, half)

            if MIDDLE <= i < MIDDLE + len(items):
                pl.when(between)(items[i - MIDDLE])

        @pl.when(patient & odd)
        def _():
            for m in range(len(pieces)):
                w_relay(m)

        @pl.when(jnp.logical_not(between))
        def _():
            w_arrive(0, first_half)
            panel_arrive()
            arrived(0, half)
            block_row(half)
            panel(half)
            update()

        @pl.when(odd & (c > 1) & jnp.logical_not(patient))
        def _():
            for m in range(FOLLOW, len(pieces)):
                w_relay(m)

        w_arrive(first_half, len(pieces))
        panel(width)
        for n in range(2):
            @pl.when(x == n)
            def _():
                finish(slice(n * width, (n + 1) * width))
                if n == 0:
                    finish_late(slice(width, 2 * width))
                else:
                    arrived(half, width)
                    finish(slice(0, width))

        @pl.when(c == 0)
        def _():
            rest_ref[:, :width] = panel_ref[...]

    @pl.when(top)
    def _():
        rest_ref[...] = jnp.zeros_like(rest_ref)

    @pl.when(corner)
    def _():
        rest_ref[:, :width] = l_ref[...]

    @pl.when(jnp.logical_not(corner))
    def _():
        log_det()

    def sent(condition, part, sem):
        @pl.when(condition)
        def _():
            send(part, part, sem, w_recv.at[0], (r, partner)).wait_send()

    inverse_part = cols_ref.at[pl.ds(0, (steps + 1) * NB // 4), :]
    sent(corner, inverse_part, w_send.at[0])
    for n, (exists, _) in enumerate(w_copies(0)):
        sent(odd & exists, inverse_part, w_send.at[n])
    for n, (exists, _) in enumerate(own_copies(0, own_part(0))):
        sent(below & even & exists, own_ref, own_send.at[n])
    for n in range(2):
        part = cols_ref.at[:, pl.ds(n * width, width)]
        sent(top & ((c > 0) | (n == 1)), part, cols_send.at[2 * n])
        for m, (exists, _) in enumerate(cols_copies(n, 0, cols_part(cols_ref, n, 0))):
            sent(below & relays[n] & exists, part, cols_send.at[2 * n + m])


def panel_step(mine):
    width = mine.shape[0]
    square = jax.ShapeDtypeStruct((width, width), jnp.float32)
    wide = (width, 2 * width)
    dma = pltpu.SemaphoreType.DMA
    pieces = (width // NB) * (width // NB + 1)
    return pl.pallas_call(
        panel_kernel,
        out_shape=(jax.ShapeDtypeStruct(wide, jnp.float32), jax.ShapeDtypeStruct((1, NB), jnp.float32)),
        in_specs=[pl.BlockSpec(memory_space=pltpu.HBM)],
        out_specs=(VMEM,) * 2,
        scratch_shapes=[
            pltpu.VMEM((width, width), jnp.float32), pltpu.VMEM(wide, jnp.float32), pltpu.VMEM((width, width), jnp.float32),
            pltpu.VMEM((width, width), jnp.float32), pltpu.VMEM(wide, jnp.float32),
            pltpu.VMEM((width, width), jnp.float32), pltpu.VMEM((width, width), jnp.float32),
            pltpu.VMEM((NB, NB), jnp.float32), pltpu.VMEM((NB, NB), jnp.float32),
            dma((2,)), dma((PANELS,)), dma((4,)), dma((2, CHUNKS)), dma((4,)), dma((pieces,)), dma(()),
        ],
        compiler_params=pltpu.CompilerParams(collective_id=0, has_side_effects=True, vmem_limit_bytes=50 << 20),
    )(mine)


def per_device(mine):
    block, logdet = panel_step(mine)
    return block, logdet[0, 0]


def solution(mesh):
    return jax.shard_map(
        per_device, mesh=mesh, in_specs=(P("row", "col"),), out_specs=(P("row", "col"), P()), check_vma=False
    )
```

```python
import functools

import jax
import jax.numpy as jnp
from jax import lax
from jax.experimental import pallas as pl
from jax.experimental.pallas import tpu as pltpu
from jax.sharding import PartitionSpec as P

MESH = pl.DeviceIdType.MESH
NB = 128
BAND = 32
CHUNKS = 32
PANELS = 16
HOPS = 2
FIRST = 2
DELAY = 3
LAST = 5
TURNS = (10, 11, 15, 16, 17, 18, 21, 21, 22, 22, 23, 24, 24, 25, 25, 26, 26, 27, 27, 28)
FOLLOW = 12
WAIT = 3
MIDDLE = 22
VMEM = pl.BlockSpec(memory_space=pltpu.VMEM)


def split(a):
    high = a.astype(jnp.bfloat16)
    return high, (a - high.astype(jnp.float32)).astype(jnp.bfloat16)


def dot_split(a, b, axis):
    def dot(u, v):
        return lax.dot_general(u, v, (((1,), (axis,)), ((), ())), preferred_element_type=jnp.float32)

    return dot(a[0], b[0]) + (dot(a[0], b[1]) + dot(a[1], b[0]))


def dot_nt(a, b):
    return dot_split(split(a), split(b), 1)


def dot_nn(a, b):
    return dot_split(split(a), split(b), 0)


def total(terms):
    while len(terms) > 1:
        terms = [a + b for a, b in zip(terms[::2], terms[1::2])]
    return terms[0]


def eliminate(left, right, base):
    sub = lax.broadcasted_iota(jnp.int32, (8, NB), 0)
    left, right = list(left), list(right)
    upper, inverse = [], []

    def row(x, t):
        return jnp.take_along_axis(x, jnp.full((8, NB), t, jnp.int32), axis=0)

    def column(x, t):
        return jnp.broadcast_to(x[:, t : t + 1], (8, NB))

    for p in range(0, len(left), 2):
        first = base + 8 * p
        rest = range(p + 2, len(left))
        cols = [[column(x, first + t) for x in left[p : p + 2]] for t in range(16)]
        mult = {g: [column(left[g], first + t) for t in range(16)] for g in rest}
        v, i = left[p : p + 2], right[p : p + 2]
        u_rows, i_rows, d_rows = list(v), list(i), [None, None]
        for t in range(16):
            at, s = t // 8, t % 8
            here = sub == s
            pivot = row(cols[t][at], s)
            if s:
                u_rows[at] = jnp.where(here, v[at], u_rows[at])
                i_rows[at] = jnp.where(here, i[at], i_rows[at])
                d_rows[at] = jnp.where(here, pivot, d_rows[at])
            else:
                u_rows[at], i_rows[at], d_rows[at] = v[at], i[at], pivot
            recip = 1.0 / pivot
            factor = [x * recip for x in cols[t]]
            factor[at] = jnp.where(here, -recip, factor[at])

            def step(pair):
                taken = row(pair[at], s)
                kept = [jnp.where(here, 0.0, x) if h == at else x for h, x in enumerate(pair)]
                return [x - f * taken for x, f in zip(kept, factor)]

            for w in range(t + 1, 16):
                cols[w] = step(cols[w])
            v, i = step(v), step(i)
        for h in range(2):
            scale = lax.rsqrt(d_rows[h])
            upper.append(u_rows[h] * scale)
            inverse.append(i_rows[h] * scale)
        v_rows = [row(v[t // 8], t % 8) for t in range(16)]
        i_rows = [row(i[t // 8], t % 8) for t in range(16)]
        for g in rest:
            left[g] = left[g] - total([mult[g][t] * v_rows[t] for t in range(16)])
            right[g] = right[g] - total([mult[g][t] * i_rows[t] for t in range(16)])
    return upper, inverse


def factor_block(a):
    lane = lax.broadcasted_iota(jnp.int32, (NB, NB), 1)
    sub = lax.broadcasted_iota(jnp.int32, (NB, NB), 0)
    left, right = a, (lane == sub).astype(jnp.float32)
    upper, inverse = [], []
    for base in range(0, NB, BAND):
        rows = [slice(8 * g, 8 * g + 8) for g in range(BAND // 8)]
        u, i = eliminate([left[x] for x in rows], [right[x] for x in rows], base)
        u, i = jnp.concatenate(u, 0), jnp.concatenate(i, 0)
        upper.append(u)
        inverse.append(i)
        if base + BAND < NB:
            change = dot_nn(u.T[base + BAND :, :], jnp.concatenate([u, i], 1))
            left, right = left[BAND:] - change[:, :NB], right[BAND:] - change[:, NB:]
    upper = jnp.where(lane >= sub, jnp.concatenate(upper, 0), 0.0)
    return upper, jnp.concatenate(inverse, 0)


def factor_all(a_ref, l_ref, w_ref, work, upper, inverse, leave):
    size = w_ref.shape[0]
    work[:NB, :NB] = a_ref[:NB, :NB]
    l_ref[...] = jnp.zeros_like(l_ref)

    @pl.loop(0, size // NB)
    def _(step):
        span = pl.ds(pl.multiple_of(step * NB, NB), NB)
        r, w = factor_block(work[span, span])
        upper[...] = r
        inverse[...] = w
        w_ref[span, span] = inverse[...]
        l_ref[span, span] = upper[...].T
        for p in range(size // NB):

            @pl.when(step == p)
            def _():
                at = slice(p * NB, (p + 1) * NB)
                end = (p + 1) * NB
                if p:
                    leave(p - 1)
                if end < size:
                    below = work[end:, at] if p else a_ref[end:, at]
                    l_ref[end:, at] = dot_nt(below, inverse[...])
                    following = slice(end, end + NB)
                    work[end:, following] = a_ref[end:, following] - dot_nt(l_ref[end:, :end], l_ref[following, :end])
                if p:
                    inner = dot_nn(l_ref[at, : p * NB], w_ref[: p * NB, : p * NB])
                    w_ref[at, : p * NB] = -dot_nn(inverse[...], inner)


def panel_kernel(mine_ref, rest_ref, logdet_ref,
                 panel_ref, other_ref, l_ref, own_ref, cols_ref, w_ref, work, upper, inverse,
                 own_send, own_recv, cols_send, cols_recv, w_send, w_recv, load_sem):
    rows, columns = lax.axis_size("row"), lax.axis_size("col")
    r, c = lax.axis_index("row"), lax.axis_index("col")
    q, x = r // 2, r % 2
    other = r + 1 - 2 * x
    partner = c + 1 - 2 * (c % 2)
    odd = c % 2 == 1
    even = jnp.logical_not(odd)
    width = own_ref.shape[0]
    top = r == 0
    below = jnp.logical_not(top)
    corner = top & (c == 0)

    links = [
        ((r, partner), partner >= 0), ((other, c), other >= 0),
        ((r - 2, c), r >= 2), ((r + 2, c), r + 2 < rows),
        ((r, c - 2), c >= 2), ((r, c + 2), c + 2 < columns),
    ]
    barrier = pltpu.get_barrier_semaphore()
    for device, exists in links:
        @pl.when(exists)
        def _():
            pl.semaphore_signal(barrier, inc=1, device_id=device, device_id_type=MESH)
    peers = sum(jnp.where(exists, 1, 0).astype(jnp.int32) for _, exists in links)
    pl.semaphore_wait(barrier, peers)

    def send(source, target, send_sem, recv_sem, device):
        return pltpu.make_async_remote_copy(
            src_ref=source, dst_ref=target, send_sem=send_sem, recv_sem=recv_sem,
            device_id=device, device_id_type=MESH,
        )

    def start(condition, copies):
        for exists, copy in copies:
            @pl.when(condition & exists)
            def _():
                copy.start()

    side_row = jnp.where(x == 0, r + 1, r - 2)
    has_side = ((x == 0) & (q >= 1)) | (r == 3)

    steps = width // NB
    tall = NB // 2
    pieces = [
        (pl.ds(p * NB + h * tall, tall), pl.ds(j * NB, NB)) for p in range(steps) for j in range(p + 1) for h in range(2)
    ]

    def row_pieces(p):
        return range(p * (p + 1), (p + 1) * (p + 2))

    def w_first(m):
        part = w_ref.at[pieces[m]]
        return send(part, part, w_send.at[0], w_recv.at[m], (r, c + 1))

    def w_copies(m):
        part = w_ref.at[pieces[m]]

        def to(n, device):
            return send(part, part, w_send.at[n], w_recv.at[m], device)

        return [
            ((c == 1) & (x == 0) & (r + 2 < rows), to(0, (r + 2, c))),
            ((c == 1) & has_side, to(1, (side_row, c))),
            (c + 2 < columns, to(2, (r, c + 2))),
            (jnp.logical_not(top & (c == 1)), to(3, (r, c - 1))),
        ]

    def w_relay(m):
        copies = w_copies(m)
        copies[0][1].wait_recv()
        start(r >= 0, copies)

    deep = width // PANELS

    def own_part(j):
        return own_ref.at[pl.ds(pl.multiple_of(j * deep, deep), deep), :]

    def own_source(j):
        return mine_ref.at[pl.ds(pl.multiple_of(j * deep, deep), deep), pl.ds(0, width)]

    def own_load(j):
        return pltpu.make_async_copy(own_source(j), own_part(j), own_recv.at[j])

    def own_copies(j, source):
        def to(n, device):
            return send(source, own_part(j), own_send.at[n], own_recv.at[j], device)

        return [(c + 2 < columns, to(0, (r, c + 2))), (c >= 0, to(1, (r, c + 1)))]

    def own_wait(j):
        own_copies(j, own_part(j))[0][1].wait_recv()

    piece = width // CHUNKS

    def cols_part(ref, n, i):
        return ref.at[pl.ds(i * piece, piece), pl.ds(n * width, width)]

    def cols_copies(n, i, source):
        def to(m, device):
            return send(source, cols_part(cols_ref, n, i), cols_send.at[2 * n + m], cols_recv.at[n, i], device)

        return [((x == n) & (r + 2 < rows), to(0, (r + 2, c))), ((x == n) & (q >= 1) | (r == 3) & (n == 0), to(1, (sides[n], c)))]

    sides = [side_row, r - 1]
    relays = [(c > 0) & (((x == 0) & (q >= 1)) | (r == 3)), x == 1]

    def cols_first(n, i):
        source = cols_part(mine_ref, n, i)
        return send(source, cols_part(cols_ref, n, i), cols_send.at[2 * n], cols_recv.at[n, i], (r + 2 - n, c))

    def cols_wait(n, i):
        cols_first(n, i).wait_recv()

    def arrived(first, last):
        for n in range(2):
            @pl.when(jnp.logical_not(relays[n]) & ((c > 0) | (n == 1)))
            def _():
                for i in range(first // piece, last // piece):
                    cols_wait(n, i)

    half = width // 2

    def log_det():
        here = lax.broadcasted_iota(jnp.int32, (NB, NB), 0) == lax.broadcasted_iota(jnp.int32, (NB, NB), 1)
        blocks = [slice(p * NB, (p + 1) * NB) for p in range(steps)]
        logs = sum(jnp.log(jnp.where(here, w_ref[at, at], 1.0)) for at in blocks)
        across = jnp.sum(logs, axis=0, keepdims=True)
        logdet_ref[...] = jnp.broadcast_to(-2.0 * jnp.sum(across, axis=1, keepdims=True), logdet_ref.shape)

    def panel(e, at=slice(None)):
        own = split(own_ref[at, :e])
        panel_ref[at, e - half : e] = dot_split(own, split(w_ref[e - half : e, :e]), 1)

    def block_row(e, at=slice(None)):
        other_ref[e - half : e, at] = dot_split(split(w_ref[e - half : e, :e]), split(cols_ref[:e, at]), 0)

    mine_load = pltpu.make_async_copy(mine_ref, rest_ref, load_sem)

    def update(at=slice(None)):
        rest_ref[:, at] = rest_ref[:, at] - dot_nn(panel_ref[:, :half], other_ref[:half, at])

    def finish(at):
        block_row(width, at)
        rest_ref[:, at] = rest_ref[:, at] - dot_nn(panel_ref[:, half:], other_ref[half:, at])

    def finish_late(at):
        last = width - NB
        arrived(half, last)
        other_ref[half:, at] = dot_nn(w_ref[half:, :last], cols_ref[:last, at])
        rest_ref[:, at] = rest_ref[:, at] - dot_nn(panel_ref[:, half:last], other_ref[half:last, at])
        arrived(last, width)
        other_ref[last:, at] = other_ref[last:, at] + dot_nn(w_ref[last:, last:], cols_ref[last:, at])
        rest_ref[:, at] = rest_ref[:, at] - dot_nn(panel_ref[:, last:], other_ref[last:, at])

    for p in range(steps):
        if p * NB % half == 0 and half > NB:
            w_ref[p * NB : (p + 1) * NB, (p + 1) * NB : p * NB + half] = jnp.zeros((NB, half - NB), jnp.float32)

    diagonal_load = pltpu.make_async_copy(mine_ref.at[:, pl.ds(0, width)], own_ref, load_sem)

    @pl.when(corner)
    def _():
        diagonal_load.start()

    @pl.when(top)
    def _():
        for i in range(CHUNKS):
            cols_first(1, i).start()

            @pl.when(c > 0)
            def _():
                cols_first(0, i).start()

    @pl.when(below & (c == 0))
    def _():
        for j in range(PANELS):
            start(c >= 0, own_copies(j, own_source(j)))
        for j in range(PANELS):
            own_load(j).start()

    @pl.when(below)
    def _():
        mine_load.start()

    def w_leave(p):
        for m in row_pieces(p):
            w_first(m).start()

    @pl.when(corner)
    def _():
        diagonal_load.wait()
        factor_all(own_ref, l_ref, w_ref, work, upper, inverse, w_leave)
        log_det()
        w_leave(steps - 1)

    @pl.when(top & odd)
    def _():
        for m in range(len(pieces)):
            w_relay(m)

    @pl.when(top & even & (c > 0))
    def _():
        for m in range(len(pieces)):
            w_first(m).wait_recv()

    first_half = row_pieces(half // NB)[0]
    patient = r == 1
    between = (x == 1) & (r + 2 >= rows)

    def w_arrive(first, last):
        @pl.when(even)
        def _():
            for m in range(first, last):
                w_first(m).wait_recv()

    def panel_arrive():
        mine_load.wait()

        @pl.when(c == 0)
        def _():
            for j in range(PANELS):
                own_load(j).wait()

        @pl.when(odd)
        def _():
            for j in range(PANELS):
                own_wait(j)

    lower = [slice(i, i + half) for i in range(0, 2 * width, half)]
    rows_of, right = lower[: width // half], lower[width // half :]
    items = [functools.partial(block_row, half, at) for at in right + rows_of]
    items += [functools.partial(panel, half, at) for at in rows_of]
    items += [functools.partial(update, at) for at in right + rows_of]

    @pl.when(below)
    def _():
        for i in range(CHUNKS):
            for n in range(2):
                @pl.when(relays[n])
                def _():
                    cols_wait(n, i)
                    start(c >= 0, cols_copies(n, i, cols_part(cols_ref, n, i)))

            for hop in range(1, HOPS + 1):
                j = i - min(FIRST + DELAY * (hop - 1), LAST)
                if 0 <= j < PANELS:
                    @pl.when(even & (c == 2 * hop if hop < HOPS else c >= 2 * hop))
                    def _():
                        own_wait(j)
                        start(c >= 0, own_copies(j, own_part(j)))

            for m, turn in enumerate(TURNS):
                for late, plane in ((0, c == 1), (WAIT, c > 1)):
                    if turn + late == i and (late == 0 or m < FOLLOW):
                        @pl.when(odd & plane & jnp.logical_not(patient))
                        def _():
                            w_relay(m)

            if i == MIDDLE:
                @pl.when(between)
                def _():
                    w_arrive(0, first_half)
                    panel_arrive()
                    arrived(0, half)

            if MIDDLE <= i < MIDDLE + len(items):
                pl.when(between)(items[i - MIDDLE])

        for first, last, plane in ((0, FOLLOW, odd), (FOLLOW, len(pieces), c == 1)):
            @pl.when(patient & plane)
            def _():
                for m in range(first, last):
                    w_relay(m)

        @pl.when(jnp.logical_not(between))
        def _():
            w_arrive(0, first_half)
            panel_arrive()
            arrived(0, half)
            block_row(half)
            panel(half)
            update()

        @pl.when(odd & (c > 1))
        def _():
            for m in range(FOLLOW, len(pieces)):
                w_relay(m)

        w_arrive(first_half, len(pieces))
        panel(width)
        for n in range(2):
            @pl.when(x == n)
            def _():
                finish(slice(n * width, (n + 1) * width))
                if n == 0:
                    finish_late(slice(width, 2 * width))
                else:
                    arrived(half, width)
                    finish(slice(0, width))

        @pl.when(c == 0)
        def _():
            rest_ref[:, :width] = panel_ref[...]

    @pl.when(top)
    def _():
        rest_ref[...] = jnp.zeros_like(rest_ref)

    @pl.when(corner)
    def _():
        rest_ref[:, :width] = l_ref[...]

    @pl.when(jnp.logical_not(corner))
    def _():
        log_det()

    def sent(condition, part, sem):
        @pl.when(condition)
        def _():
            send(part, part, sem, w_recv.at[0], (r, partner)).wait_send()

    inverse_part = cols_ref.at[pl.ds(0, (steps + 1) * NB // 4), :]
    sent(corner, inverse_part, w_send.at[0])
    for n, (exists, _) in enumerate(w_copies(0)):
        sent(odd & exists, inverse_part, w_send.at[n])
    for n, (exists, _) in enumerate(own_copies(0, own_part(0))):
        sent(below & even & exists, own_ref, own_send.at[n])
    for n in range(2):
        part = cols_ref.at[:, pl.ds(n * width, width)]
        sent(top & ((c > 0) | (n == 1)), part, cols_send.at[2 * n])
        for m, (exists, _) in enumerate(cols_copies(n, 0, cols_part(cols_ref, n, 0))):
            sent(below & relays[n] & exists, part, cols_send.at[2 * n + m])


def panel_step(mine):
    width = mine.shape[0]
    square = jax.ShapeDtypeStruct((width, width), jnp.float32)
    wide = (width, 2 * width)
    dma = pltpu.SemaphoreType.DMA
    pieces = (width // NB) * (width // NB + 1)
    return pl.pallas_call(
        panel_kernel,
        out_shape=(jax.ShapeDtypeStruct(wide, jnp.float32), jax.ShapeDtypeStruct((1, NB), jnp.float32)),
        in_specs=[pl.BlockSpec(memory_space=pltpu.HBM)],
        out_specs=(VMEM,) * 2,
        scratch_shapes=[
            pltpu.VMEM((width, width), jnp.float32), pltpu.VMEM(wide, jnp.float32), pltpu.VMEM((width, width), jnp.float32),
            pltpu.VMEM((width, width), jnp.float32), pltpu.VMEM(wide, jnp.float32),
            pltpu.VMEM((width, width), jnp.float32), pltpu.VMEM((width, width), jnp.float32),
            pltpu.VMEM((NB, NB), jnp.float32), pltpu.VMEM((NB, NB), jnp.float32),
            dma((2,)), dma((PANELS,)), dma((4,)), dma((2, CHUNKS)), dma((4,)), dma((pieces,)), dma(()),
        ],
        compiler_params=pltpu.CompilerParams(collective_id=0, has_side_effects=True, vmem_limit_bytes=50 << 20),
    )(mine)


def per_device(mine):
    block, logdet = panel_step(mine)
    return block, logdet[0, 0]


def solution(mesh):
    return jax.shard_map(
        per_device, mesh=mesh, in_specs=(P("row", "col"),), out_specs=(P("row", "col"), P()), check_vma=False
    )
```
